512 devices in a mesh: freq: 16 (over x, z_lo), line: 32 (over z_hi, y, core).
Axes of the slice: x: 4, y: 4, z: 16 (z_hi: 4, z_lo: 4; z = z_hi * 4 + z_lo), core: 2. Of those that a mesh axis runs over, the one named last changes fastest.
Arguments:
- field: float32 [16, 2, 4, 96, 64, 256], P('freq', None, None, None, 'line'), may hold values from -6 to 6
- live_count: int32 [64], P('line'), may hold values from 64 to 256
- line_owner: int32 [64], replicated, may hold values from 0 to 63, each once
- decomposer: float32 [16, 2, 4, 4, 64, 256], P('freq', None, None, None, 'line'), may hold values from -1.4 to 2.4
- reflection: bfloat16 [16, 1024, 2, 16384], P('freq', None, None, 'line'), may hold values from -0.0625 to 0.0625
- direct_wave: float32 [1024, 16, 2, 384], P('line', 'freq'), may hold values from -6 to 6
Outputs:
- focusing: float32 [1024, 16, 2, 384], P('line', 'freq')
- trace_energy: float32 [1024], P('line')
The draws below stay inside these ranges and needn't reach their ends.
Inputs may be any that keep to these rules, and one draw needn't show every extreme that they name: `line_owner`: each crossline position appears once.
All inputs are finite; a program needn't handle non-finite values.
Results may differ from the reference program's by a relative error of at most 0.0023.
Values may be sent and summed in bfloat16 or wider, within the bound.
No kernel may reach another device: no remote copies, remote signals or barrier semaphores. Data moves between devices by JAX's collectives and lax.ppermute only.
A program may use at most 64 MiB of HBM per device.

```python
import math
import jax
import jax.numpy as jnp
from jax import lax

LINES = 64
RCV = 256
FREQS = 16
FOCI = 96
SRC = 1024


def draw_decomposer(key, part):
    shape = (FREQS, 2, 4, 4, LINES, RCV)
    noise = jnp.clip(0.35 * jax.random.normal(key, shape, jnp.float32), -1.4, 1.4)
    identity = jnp.eye(4, dtype=jnp.float32)
    diagonal_part = jnp.stack([identity, jnp.zeros((4, 4), jnp.float32)])
    return noise + diagonal_part[None, :, :, :, None, None]


def touch_ends(result, key, low, high):
    shape = result.shape
    index_at = [jax.random.randint(jax.random.fold_in(key, axis), (), 0, shape[axis]) for axis in range(len(shape))]
    result = result.at[tuple(index_at)].set(low)
    longest = shape.index(max(shape))
    index_at[longest] = (index_at[longest] + 1) % shape[longest]
    return result.at[tuple(index_at)].set(high)


def raised(values, rng, source, target, parts, factor):
    def block_of(dim):
        return (jnp.arange(values.shape[dim]) // (values.shape[dim] // parts)).reshape((-1,) + (1,) * (values.ndim - 1 - dim))

    one_side = jax.random.permutation(rng, parts)[block_of(target)]
    second = (block_of(target) + parts // 2) % parts
    return jnp.where((block_of(source) == one_side) | (block_of(source) == second), factor * values, values)


def steps_of(rng, shape, cuts, smallest, top_value):
    loudness = 1.0
    for position, parts in cuts:
        draws = jax.random.uniform(jax.random.fold_in(jax.random.fold_in(rng, 6), position), (parts,), jnp.float32, smallest / len(cuts), top_value / len(cuts))
        loudness = loudness * jnp.repeat(jnp.exp(draws), shape[position] // parts).reshape((-1,) + (1,) * (len(shape) - 1 - position))
    return loudness


def normal_values(stream_key, dims, scale, reach, split=(), held_as=jnp.bfloat16):
    loudness = steps_of(stream_key, dims, split, -0.22, 0.18) if split else 1.0
    drawn = jax.random.normal(stream_key, dims, jnp.float32) * scale * loudness
    return jnp.minimum(jnp.maximum(drawn, -reach), reach).astype(held_as)


def heavy_noise(stream_key, shape, scale, most, split, heavy, kind=jnp.bfloat16):
    result = scale * jax.random.normal(stream_key, shape, jnp.float32)
    if split:
        result = result * steps_of(stream_key, shape, split, -0.22, 0.18)
    return jnp.clip(raised(result, jax.random.fold_in(stream_key, 3), *heavy), -most, most).astype(kind)


def setup_inputs(seed: int = 0) -> dict:
    key_list = jax.random.split(jax.random.key(seed), 7)
    return {
        "field": normal_values(key_list[0], (FREQS, 2, 4, FOCI, LINES, RCV), 1.0, 6.0, ((0, 16), (4, 32)), jnp.float32),
        "live_count": touch_ends(jax.random.randint(key_list[1], (LINES,), RCV // 4, RCV + 1), jax.random.fold_in(key_list[1], 1), RCV // 4, RCV).astype(jnp.int32),
        "line_owner": jax.random.permutation(key_list[2], LINES).astype(jnp.int32),
        "decomposer": draw_decomposer(jax.random.fold_in(key_list[6], 71), 0),
        "reflection": heavy_noise(key_list[4], (FREQS, SRC, 2, LINES * RCV), (2 * LINES * RCV) ** -0.5, 0.0625, ((0, 16), (3, 32)), (3, 1, 32, 2.75)),
        "direct_wave": normal_values(key_list[5], (SRC, FREQS, 2, 4 * FOCI), 1.0, 6.0, ((0, 32), (1, 16)), jnp.float32),
    }


def phase_tables(line_owner, length):
    wavenum = jnp.arange(length, dtype=jnp.int32)
    products = wavenum[:, None] * line_owner[None, :].astype(jnp.int32) % length
    angles = products.astype(jnp.float32) * (2.0 * math.pi / length)
    return (jnp.cos(angles), jnp.sin(angles))

def decompose(operator, spectrum):
    real_rows = []
    imag_rows = []
    for target in range(4):
        real_sum = None
        imag_sum = None
        for source in range(4):
            weight_real = operator[:, 0, target, source][:, None]
            weight_imag = operator[:, 1, target, source][:, None]
            field_real = spectrum[:, 0, source]
            field_imag = spectrum[:, 1, source]
            term_real = weight_real * field_real - weight_imag * field_imag
            term_imag = weight_real * field_imag + weight_imag * field_real
            real_sum = term_real if real_sum is None else real_sum + term_real
            imag_sum = term_imag if imag_sum is None else imag_sum + term_imag
        real_rows.append(real_sum)
        imag_rows.append(imag_sum)
    return jnp.stack([jnp.stack(real_rows, 1), jnp.stack(imag_rows, 1)], 1)

def reference(field, live_count, line_owner, decomposer, reflection, direct_wave):
    cosine, sine_table = phase_tables(line_owner, LINES)
    forward_table = jnp.stack([jnp.stack([cosine, sine_table]), jnp.stack([-sine_table, cosine])])
    inverse_table = jnp.stack([jnp.stack([cosine.T, -sine_table.T]), jnp.stack([sine_table.T, cosine.T])]) / LINES
    live_mask = jnp.arange(RCV, dtype=jnp.int32)[None, :] < live_count[:, None]

    def one_freq(operands):
        block, operator, panel = operands
        live_field = jnp.where(live_mask, block, jnp.float32(0.0))
        spectrum = jnp.einsum('yxkj,xiojr->yiokr', forward_table, live_field, precision=lax.Precision.HIGHEST)
        decomposed = decompose(operator[None], spectrum[None])[0]
        wavefield = jnp.einsum('yxjk,xiokr->yiojr', inverse_table, decomposed, precision=lax.Precision.HIGHEST)
        wave_bf = wavefield.astype(jnp.bfloat16).reshape(2, 4 * FOCI, LINES * RCV)
        real_part = wave_bf[0]
        imag_part = wave_bf[1]
        stacked = jnp.stack([jnp.stack([real_part, imag_part], 0), jnp.stack([-imag_part, real_part], 0)], 0)
        right_side = jnp.transpose(stacked, (0, 3, 1, 2)).reshape(2 * LINES * RCV, 8 * FOCI)
        left_side = panel.reshape(SRC, 2 * LINES * RCV)
        product = jnp.dot(left_side, right_side, preferred_element_type=jnp.float32)
        return product.reshape(SRC, 2, 4 * FOCI)
    reflected = lax.map(one_freq, (field, decomposer, reflection))
    reflected = jnp.transpose(reflected, (1, 0, 2, 3))
    focusing = direct_wave - reflected
    weights = 2.0 * jnp.arange(1, FREQS + 1, dtype=jnp.int32).astype(jnp.float32) / (FREQS * (FREQS + 1))
    energy_sum = lax.optimization_barrier(jnp.sum(lax.optimization_barrier(jnp.sum(reflected * reflected, axis=(2, 3))) * weights[None, :], axis=1))
    trace_energy = jnp.sqrt(energy_sum / (8 * FOCI) + 1e-06)
    return (focusing, trace_energy)
```

```python
import math

import jax
import jax.numpy as jnp
from jax import lax
from jax.experimental import pallas as pl
from jax.experimental.pallas import tpu as pltpu
from jax.sharding import Mesh
from jax.sharding import PartitionSpec as P

LINE = ("line_0", "line_1", "line_2")
LOW_SCALE = 2048.0


def phase_tables(line_owner, length):
    wavenum = jnp.arange(length, dtype=jnp.int32)
    owner = line_owner.reshape(32, 2).T.reshape(64)
    wavenum = wavenum.reshape(32, 2).T.reshape(64)
    products = wavenum[:, None] * owner[None, :] % length
    angles = products.astype(jnp.float32) * (2.0 * math.pi / length)
    return (jnp.cos(angles), jnp.sin(angles))


def in_two_terms(table):
    high = table.astype(jnp.bfloat16)
    low = (table - high.astype(jnp.float32)).astype(jnp.bfloat16)
    return jnp.concatenate(
        [jnp.concatenate([high, high], 1), jnp.concatenate([low, low], 1)], 0
    )


def transform_tables(line_owner):
    length = line_owner.shape[0]
    cosine, sine = phase_tables(line_owner, length)
    forward = jnp.stack([jnp.stack([cosine, sine]), jnp.stack([-sine, cosine])])
    forward = forward.reshape(2, 2, 64, 2, 32).transpose(0, 2, 3, 1, 4).reshape(128, 128)
    inverse = jnp.stack([jnp.stack([cosine.T, -sine.T]), jnp.stack([sine.T, cosine.T])]) / length
    inverse = inverse.reshape(2, 2, 2, 32, 64).transpose(2, 0, 3, 1, 4).reshape(128, 128)
    return in_two_terms(forward), in_two_terms(inverse)


def middle_kernel(message_ref, forward_ref, inverse_ref, out_ref, wave_ref):
    lane = lax.broadcasted_iota(jnp.int32, (64, 128), 1)
    forward = forward_ref[...]
    inverse = inverse_ref[...]

    def transform(table, value):
        high = value.astype(jnp.bfloat16)
        low = (value - high.astype(jnp.float32)).astype(jnp.bfloat16)
        both = jnp.dot(
            table, jnp.concatenate([high, low], 0), preferred_element_type=jnp.float32
        )
        return both[:128] + both[128:]

    for r in range(8):
        tiles = [
            jnp.concatenate(
                [message_ref[pl.ds((g * 3 + t) * 8 + r, 32, stride=104), :] for g in range(4)], 0
            )
            for t in range(3)
        ]
        spectrum = transform(forward, jnp.concatenate(tiles, 1))
        operator = message_ref[pl.ds(96 + r, 32, stride=104), :]
        operator = operator + pltpu.roll(operator, 64, 1) * jnp.float32(1.0 / LOW_SCALE)
        operator = jnp.concatenate([operator, pltpu.roll(operator, 96, 1)], 0)
        parts = []
        for part in range(2):
            t0, t1, t2 = [
                spectrum[64 * part : 64 * part + 64, 128 * t : 128 * t + 128] for t in range(3)
            ]
            parts.append(
                [
                    t0,
                    pltpu.roll(jnp.where(lane >= 96, t0, t1), 32, 1),
                    pltpu.roll(jnp.where(lane >= 64, t1, t2), 64, 1),
                    pltpu.roll(t2, 96, 1),
                ]
            )
        rows = [[], []]
        for target in range(4):
            real_sum = None
            imag_sum = None
            for source in range(4):
                at = target * 4 + source
                weight_real = operator[:, at : at + 1]
                weight_imag = operator[:, 16 + at : 17 + at]
                field_real = parts[0][source]
                field_imag = parts[1][source]
                term_real = weight_real * field_real - weight_imag * field_imag
                term_imag = weight_real * field_imag + weight_imag * field_real
                real_sum = term_real if real_sum is None else real_sum + term_real
                imag_sum = term_imag if imag_sum is None else imag_sum + term_imag
            rows[0].append(real_sum)
            rows[1].append(imag_sum)
        decomposed = []
        for part in range(2):
            q0, q1, q2, q3 = rows[part]
            q1 = pltpu.roll(q1, 96, 1)
            q2 = pltpu.roll(q2, 64, 1)
            q3 = pltpu.roll(q3, 32, 1)
            decomposed.append(
                jnp.concatenate(
                    [
                        jnp.where(lane < 96, q0, q1),
                        jnp.where(lane < 64, q1, q2),
                        jnp.where(lane < 32, q2, q3),
                    ],
                    1,
                )
            )
        wave = transform(inverse, jnp.concatenate(decomposed, 0))
        for g in range(4):
            for t in range(3):
                wave_ref[pl.ds((g * 3 + t) * 8 + r, 32, stride=96), :] = wave[
                    32 * g : 32 * g + 32, 128 * t : 128 * t + 128
                ]
    out_ref[...] = wave_ref[...].reshape(32, 12, 8, 128).astype(jnp.bfloat16)


def middle(message, forward, inverse):
    return pl.pallas_call(
        middle_kernel,
        out_shape=jax.ShapeDtypeStruct((32, 12, 8, 128), jnp.bfloat16),
        in_specs=[pl.BlockSpec(memory_space=pltpu.VMEM)] * 3,
        out_specs=pl.BlockSpec(memory_space=pltpu.VMEM),
        scratch_shapes=[pltpu.VMEM((3072, 128), jnp.float32)],
    )(message.astype(jnp.float32).reshape(3328, 128), forward, inverse)


def outgoing(field, live_count, decomposer):
    receivers = field.shape[5]
    live_mask = jnp.arange(receivers, dtype=jnp.int32)[None, :] < live_count[:, None]
    live_field = jnp.where(live_mask, field[0], jnp.float32(0.0)).astype(jnp.float16)
    live_field = live_field.reshape(2, 384, 2, 32, 8)
    live_field = live_field.transpose(3, 2, 0, 4, 1).reshape(32, 2, 2, 8, 3, 128)
    live_field = live_field.transpose(0, 1, 2, 4, 3, 5).reshape(32, 12, 8, 128)
    operator = decomposer[0].reshape(32, 2, 256).transpose(2, 1, 0).reshape(32, 1, 8, 64)
    high = operator.astype(jnp.float16)
    low = ((operator - high.astype(jnp.float32)) * LOW_SCALE).astype(jnp.float16)
    return jnp.concatenate([live_field, jnp.concatenate([high, low], 3)], 1)


def summed(blocks, axis, scale):
    count = lax.axis_size(axis)
    blocks = (blocks * scale).astype(jnp.float16).reshape(count, -1, blocks.shape[-1])
    blocks = lax.all_to_all(blocks, axis, 0, 0, tiled=True)
    return blocks.astype(jnp.float32).sum(axis=0) * (1.0 / scale)


def over_copies(shard, axis):
    count = lax.axis_size(axis)
    shards = jnp.broadcast_to(shard[None], (count, *shard.shape))
    return lax.all_to_all(shards, axis, 0, 0, tiled=True).sum(axis=0)


def on_device(field, live_count, line_owner, decomposer, reflection, direct_wave):
    forward, inverse = transform_tables(line_owner)
    message = outgoing(field, live_count, decomposer)
    message = lax.all_to_all(message, LINE, 0, 0, tiled=True)
    wave = lax.all_to_all(middle(message, forward, inverse), LINE, 0, 0, tiled=True)
    wave = wave.reshape(32, 2, 2, 3, 8, 128).transpose(2, 1, 0, 4, 3, 5).reshape(2, 512, 384)
    panel = reflection[0].reshape(4, 4, 2, 32, 1024).transpose(2, 1, 0, 3, 4).reshape(1024, 1024)
    stacked = jnp.concatenate(
        [jnp.concatenate([wave[0], wave[1]], 1), jnp.concatenate([-wave[1], wave[0]], 1)], 0
    )
    product = jnp.dot(panel, stacked, preferred_element_type=jnp.float32)
    product = summed(product, "line_2", 1.0)
    product = summed(product, "line_1", 0.5)
    product = summed(product, "line_0", 0.125)
    reflected = product.reshape(32, 1, 2, 384)
    focusing = direct_wave - reflected
    total_freqs = lax.axis_size("freq")
    weight = 2.0 * (lax.axis_index("freq") + 1).astype(jnp.float32) / (total_freqs * (total_freqs + 1))
    partial_value = jnp.sum(reflected * reflected, axis=(1, 2, 3)) * weight
    energy_sum = over_copies(partial_value, "freq")
    trace_energy = jnp.sqrt(energy_sum / 768 + 1e-06)
    return (focusing, trace_energy)


def solution(mesh):
    finer = Mesh(
        mesh.devices.reshape(mesh.shape["freq"], 4, 4, 2), ("freq", "line_0", "line_1", "line_2")
    )
    in_specs = (
        P("freq", None, None, None, LINE, None),
        P(LINE),
        P(),
        P("freq", None, None, None, LINE, None),
        P("freq", None, None, LINE),
        P(LINE, "freq", None, None),
    )
    out_specs = (P(LINE, "freq", None, None), P(LINE))
    return jax.shard_map(
        on_device, mesh=finer, in_specs=in_specs, out_specs=out_specs, check_vma=False
    )
```

```python
import math

import jax
import jax.numpy as jnp
from jax import lax
from jax.experimental import pallas as pl
from jax.experimental.pallas import tpu as pltpu
from jax.sharding import Mesh
from jax.sharding import PartitionSpec as P

LINE = ("line_0", "line_1", "line_2")
RECEIVER = ("line_1", "line_2", "line_0")
PLANE = ("line_1", "line_2")
LOW_SCALE = 2048.0


def by_receiver_owner(values):
    return values.reshape(4, 4, 2, 2).transpose(3, 1, 2, 0).reshape(64)


def by_line_owner(values):
    return values.reshape(32, 2).T.reshape(64)


def phases(wavenum, owner):
    products = wavenum[:, None] * owner[None, :] % 64
    angles = products.astype(jnp.float32) * (2.0 * math.pi / 64)
    return (jnp.cos(angles), jnp.sin(angles))


def in_two_terms(table):
    high = lax.reduce_precision(table, 8, 7)
    low = lax.reduce_precision(table - high, 8, 7)
    high = high.astype(jnp.bfloat16)
    low = low.astype(jnp.bfloat16)
    return jnp.concatenate(
        [jnp.concatenate([high, high], 1), jnp.concatenate([low, low], 1)], 0
    )


def transform_tables(line_owner):
    wavenum = by_receiver_owner(jnp.arange(64, dtype=jnp.int32))
    cosine, sine = phases(wavenum, by_receiver_owner(line_owner))
    forward = jnp.stack([jnp.stack([cosine, sine]), jnp.stack([-sine, cosine])])
    forward = forward.reshape(2, 2, 64, 2, 32).transpose(0, 2, 3, 1, 4).reshape(128, 128)
    cosine, sine = phases(wavenum, by_line_owner(line_owner))
    inverse = jnp.stack([jnp.stack([cosine.T, -sine.T]), jnp.stack([sine.T, cosine.T])]) / 64
    inverse = inverse.reshape(2, 2, 2, 32, 64).transpose(2, 0, 3, 1, 4).reshape(128, 128)
    return in_two_terms(forward), in_two_terms(inverse)


def middle_kernel(message_ref, forward_ref, inverse_ref, out_ref, wave_ref):
    lane = lax.broadcasted_iota(jnp.int32, (64, 128), 1)
    forward = forward_ref[...]
    inverse = inverse_ref[...]

    def transform(table, value):
        high = value.astype(jnp.bfloat16)
        low = (value - high.astype(jnp.float32)).astype(jnp.bfloat16)
        both = jnp.dot(
            table, jnp.concatenate([high, low], 0), preferred_element_type=jnp.float32
        )
        return both[:128] + both[128:]

    for r in range(8):
        tiles = [
            jnp.concatenate(
                [message_ref[pl.ds((g * 3 + t) * 8 + r, 32, stride=104), :] for g in range(4)], 0
            )
            for t in range(3)
        ]
        spectrum = transform(forward, jnp.concatenate(tiles, 1))
        operator = message_ref[pl.ds(96 + r, 32, stride=104), :]
        operator = operator + pltpu.roll(operator, 64, 1) * jnp.float32(1.0 / LOW_SCALE)
        operator = jnp.concatenate([operator, pltpu.roll(operator, 96, 1)], 0)
        parts = []
        for part in range(2):
            t0, t1, t2 = [
                spectrum[64 * part : 64 * part + 64, 128 * t : 128 * t + 128] for t in range(3)
            ]
            parts.append(
                [
                    t0,
                    pltpu.roll(jnp.where(lane >= 96, t0, t1), 32, 1),
                    pltpu.roll(jnp.where(lane >= 64, t1, t2), 64, 1),
                    pltpu.roll(t2, 96, 1),
                ]
            )
        rows = [[], []]
        for target in range(4):
            real_sum = None
            imag_sum = None
            for source in range(4):
                at = target * 4 + source
                weight_real = operator[:, at : at + 1]
                weight_imag = operator[:, 16 + at : 17 + at]
                field_real = parts[0][source]
                field_imag = parts[1][source]
                term_real = weight_real * field_real - weight_imag * field_imag
                term_imag = weight_real * field_imag + weight_imag * field_real
                real_sum = term_real if real_sum is None else real_sum + term_real
                imag_sum = term_imag if imag_sum is None else imag_sum + term_imag
            rows[0].append(real_sum)
            rows[1].append(imag_sum)
        decomposed = []
        for part in range(2):
            q0, q1, q2, q3 = rows[part]
            q1 = pltpu.roll(q1, 96, 1)
            q2 = pltpu.roll(q2, 64, 1)
            q3 = pltpu.roll(q3, 32, 1)
            decomposed.append(
                jnp.concatenate(
                    [
                        jnp.where(lane < 96, q0, q1),
                        jnp.where(lane < 64, q1, q2),
                        jnp.where(lane < 32, q2, q3),
                    ],
                    1,
                )
            )
        wave = transform(inverse, jnp.concatenate(decomposed, 0))
        for g in range(4):
            for t in range(3):
                wave_ref[pl.ds((g * 3 + t) * 8 + r, 32, stride=96), :] = wave[
                    32 * g : 32 * g + 32, 128 * t : 128 * t + 128
                ]
    out_ref[...] = wave_ref[...].reshape(32, 12, 8, 128).astype(jnp.bfloat16)


def middle(message, forward, inverse):
    return pl.pallas_call(
        middle_kernel,
        out_shape=jax.ShapeDtypeStruct((32, 12, 8, 128), jnp.bfloat16),
        in_specs=[pl.BlockSpec(memory_space=pltpu.VMEM)] * 3,
        out_specs=pl.BlockSpec(memory_space=pltpu.VMEM),
        scratch_shapes=[pltpu.VMEM((3072, 128), jnp.float32)],
    )(message.astype(jnp.float32).reshape(3328, 128), forward, inverse)


def outgoing(field, live_count, decomposer):
    receivers = field.shape[5]
    live_mask = jnp.arange(receivers, dtype=jnp.int32)[None, :] < live_count[:, None]
    live_field = jnp.where(live_mask, field[0], jnp.float32(0.0)).astype(jnp.float16)
    live_field = live_field.reshape(2, 384, 2, 32, 8)
    live_field = live_field.transpose(3, 2, 0, 4, 1).reshape(32, 2, 2, 8, 3, 128)
    live_field = live_field.transpose(0, 1, 2, 4, 3, 5).reshape(32, 12, 8, 128)
    operator = decomposer[0].reshape(32, 2, 256).transpose(2, 1, 0).reshape(32, 1, 8, 64)
    high = operator.astype(jnp.float16)
    low = ((operator - high.astype(jnp.float32)) * LOW_SCALE).astype(jnp.float16)
    return jnp.concatenate([live_field, jnp.concatenate([high, low], 3)], 1)


def panel_blocks(reflection):
    panel = reflection[0].reshape(4, 4, 2, 32, 1024).transpose(2, 1, 0, 3, 4).reshape(1024, 1024)
    taken = jnp.arange(1024, dtype=jnp.int32)
    part, line, device, receiver = taken // 512, taken // 256 % 2, taken // 32 % 8, taken % 32
    place = ((device * 2 + part) * 2 + line) * 32 + receiver
    moved = (place[:, None] == taken[None, :]).astype(jnp.bfloat16)
    panel = jnp.dot(panel, moved, preferred_element_type=jnp.float32).astype(jnp.bfloat16)
    return panel.reshape(1024, 8, 128).transpose(1, 0, 2)


def exchanged(blocks):
    rank = lax.axis_index(PLANE)
    received = [lax.dynamic_index_in_dim(blocks, rank, keepdims=False)]
    for distance in range(1, 8):
        block = lax.dynamic_index_in_dim(blocks, rank ^ distance, keepdims=False)
        pairs = [(i, i ^ distance) for i in range(8)]
        received.append(lax.ppermute(block, PLANE, pairs))
    return received


def panel_halves(received):
    rank = lax.axis_index(PLANE)
    core = lax.axis_index("line_2")
    stack = jnp.stack(received)
    halves = []
    for half in (1 - core, core):
        rows = [
            lax.dynamic_slice(stack, (rank ^ source, half * 512, 0), (1, 512, 128))[0]
            for source in range(8)
        ]
        halves.append(jnp.concatenate(rows, 1))
    return halves


def summed(blocks, axis, scale):
    count = lax.axis_size(axis)
    blocks = (blocks * scale).astype(jnp.float16).reshape(count, -1, blocks.shape[-1])
    blocks = lax.all_to_all(blocks, axis, 0, 0, tiled=True)
    return blocks.astype(jnp.float32).sum(axis=0) * (1.0 / scale)


def over_copies(shard, axis):
    count = lax.axis_size(axis)
    shards = jnp.broadcast_to(shard[None], (count, *shard.shape))
    return lax.all_to_all(shards, axis, 0, 0, tiled=True).sum(axis=0)


def on_device(field, live_count, line_owner, decomposer, reflection, direct_wave):
    forward, inverse = transform_tables(line_owner)
    total_freqs = lax.axis_size("freq")
    weight = 2.0 * (lax.axis_index("freq") + 1).astype(jnp.float32) / (total_freqs * (total_freqs + 1))
    weight = jnp.full((32,), weight)
    message = outgoing(field, live_count, decomposer)
    message, reflection, weight = lax.optimization_barrier((message, reflection, weight))
    message = lax.all_to_all(message, RECEIVER, 0, 0, tiled=True)
    received = exchanged(panel_blocks(reflection))
    wave = middle(message, forward, inverse)
    wave = lax.all_to_all(wave, "line_0", 0, 0, tiled=True)
    other_panel, own_panel = panel_halves(received)
    wave = wave.reshape(4, 8, 2, 2, 3, 8, 128).transpose(3, 1, 2, 0, 5, 4, 6).reshape(2, 8, 64, 384)
    stacked = jnp.stack(
        [jnp.concatenate([wave[0], wave[1]], 2), jnp.concatenate([-wave[1], wave[0]], 2)], 1
    ).reshape(1024, 768)
    sent = jnp.dot(other_panel, stacked, preferred_element_type=jnp.float32).astype(jnp.float16)
    sent = lax.ppermute(sent, "line_2", [(0, 1), (1, 0)])
    product = jnp.dot(own_panel, stacked, preferred_element_type=jnp.float32)
    product = product + sent.astype(jnp.float32)
    product = summed(product, "line_1", 0.5)
    product = summed(product, "line_0", 0.125)
    reflected = product.reshape(32, 1, 2, 384)
    focusing = direct_wave - reflected
    partial_value = jnp.sum(reflected * reflected, axis=(1, 2, 3)) * weight
    focusing, partial_value = lax.optimization_barrier((focusing, partial_value))
    energy_sum = over_copies(partial_value, "freq")
    trace_energy = jnp.sqrt(energy_sum / 768 + 1e-06)
    return (focusing, trace_energy)


def solution(mesh):
    finer = Mesh(
        mesh.devices.reshape(mesh.shape["freq"], 4, 4, 2), ("freq", "line_0", "line_1", "line_2")
    )
    in_specs = (
        P("freq", None, None, None, LINE, None),
        P(LINE),
        P(),
        P("freq", None, None, None, LINE, None),
        P("freq", None, None, LINE),
        P(LINE, "freq", None, None),
    )
    out_specs = (P(LINE, "freq", None, None), P(LINE))
    return jax.shard_map(
        on_device, mesh=finer, in_specs=in_specs, out_specs=out_specs, check_vma=False
    )
```

```python
import math

import jax
import jax.numpy as jnp
from jax import lax
from jax.experimental import pallas as pl
from jax.experimental.pallas import tpu as pltpu
from jax.sharding import Mesh
from jax.sharding import PartitionSpec as P

LINE = ("line_0", "line_1", "line_2")
RECEIVER = ("line_1", "line_2", "line_0")
PLANE = ("line_1", "line_2")
LOW_SCALE = 256.0


def by_receiver_owner(values):
    return values.reshape(4, 4, 2, 2).transpose(3, 1, 2, 0).reshape(64)


def by_line_owner(values):
    return values.reshape(32, 2).T.reshape(64)


def phases(wavenum, owner):
    products = wavenum[:, None] * owner[None, :] % 64
    angles = products.astype(jnp.float32) * (2.0 * math.pi / 64)
    return (jnp.cos(angles), jnp.sin(angles))


def in_two_terms(table):
    high = lax.reduce_precision(table, 8, 7)
    low = lax.reduce_precision(table - high, 8, 7)
    high = high.astype(jnp.bfloat16)
    low = low.astype(jnp.bfloat16)
    return jnp.concatenate(
        [jnp.concatenate([high, high], 1), jnp.concatenate([low, low], 1)], 0
    )


def transform_tables(line_owner):
    wavenum = by_receiver_owner(jnp.arange(64, dtype=jnp.int32))
    cosine, sine = phases(wavenum, by_receiver_owner(line_owner))
    forward = jnp.stack([jnp.stack([cosine, sine]), jnp.stack([-sine, cosine])])
    forward = forward.transpose(0, 2, 1, 3).reshape(128, 128)
    cosine, sine = phases(wavenum, by_line_owner(line_owner))
    inverse = jnp.stack([jnp.stack([cosine.T, -sine.T]), jnp.stack([sine.T, cosine.T])]) / 64
    inverse = inverse.reshape(2, 2, 2, 32, 64).transpose(2, 0, 3, 1, 4).reshape(128, 128)
    return in_two_terms(forward), in_two_terms(inverse)


def spread_table():
    row = jnp.arange(128, dtype=jnp.int32)[:, None]
    column = jnp.arange(2048, dtype=jnp.int32)[None, :]
    low, line, part, target, source = row // 64, row // 32 % 2, row // 16 % 2, row // 4 % 4, row % 4
    shift, goal = column // 128 % 4, column // 32 % 4
    found = (line == column // 1024) & (part == column // 512 % 2) & (target == goal)
    found = found & (source == (goal - shift) % 4)
    return jnp.where(found, jnp.where(low == 1, 1.0 / LOW_SCALE, 1.0), 0.0).astype(jnp.bfloat16)


def middle_kernel(message_ref, forward_ref, inverse_ref, spread_ref, out_ref, wave_ref, spread_out_ref):
    forward = forward_ref[...]
    inverse = inverse_ref[...]
    operators = jnp.concatenate(
        [message_ref[pl.ds(96 + r, 32, stride=104), :] for r in range(8)], 0
    ).astype(jnp.bfloat16)
    spread_out_ref[...] = jnp.dot(operators, spread_ref[...], preferred_element_type=jnp.float32)

    def transform(table, value):
        high = value.astype(jnp.bfloat16)
        low = (value - high.astype(jnp.float32)).astype(jnp.bfloat16)
        both = jnp.dot(
            table, jnp.concatenate([high, low], 0), preferred_element_type=jnp.float32
        )
        return both[:128] + both[128:]

    for r in range(8):
        tiles = [
            jnp.concatenate(
                [message_ref[pl.ds((g * 3 + t) * 8 + r, 32, stride=104), :] for g in range(4)], 0
            )
            for t in range(3)
        ]
        spectrum = transform(forward, jnp.concatenate(tiles, 1))
        decomposed = []
        for t in range(3):
            field_real = spectrum[:64, 128 * t : 128 * t + 128]
            field_imag = spectrum[64:, 128 * t : 128 * t + 128]
            real_sum = None
            imag_sum = None
            for shift in range(4):
                weight_real, weight_imag = [
                    jnp.concatenate(
                        [
                            spread_out_ref[
                                32 * r : 32 * r + 32, pl.ds(1024 * line + 512 * part + 128 * shift, 128)
                            ]
                            for line in range(2)
                        ],
                        0,
                    )
                    for part in range(2)
                ]
                moved_real = pltpu.roll(field_real, 32 * shift, 1) if shift else field_real
                moved_imag = pltpu.roll(field_imag, 32 * shift, 1) if shift else field_imag
                term_real = weight_real * moved_real - weight_imag * moved_imag
                term_imag = weight_real * moved_imag + weight_imag * moved_real
                real_sum = term_real if real_sum is None else real_sum + term_real
                imag_sum = term_imag if imag_sum is None else imag_sum + term_imag
            decomposed.append(jnp.concatenate([real_sum, imag_sum], 0))
        wave = transform(inverse, jnp.concatenate(decomposed, 1))
        for g in range(4):
            for t in range(3):
                wave_ref[pl.ds((g * 3 + t) * 8 + r, 32, stride=96), :] = wave[
                    32 * g : 32 * g + 32, 128 * t : 128 * t + 128
                ]
    out_ref[...] = wave_ref[...].reshape(32, 12, 8, 128).astype(jnp.bfloat16)


def middle(message, forward, inverse, spread):
    return pl.pallas_call(
        middle_kernel,
        out_shape=jax.ShapeDtypeStruct((32, 12, 8, 128), jnp.bfloat16),
        in_specs=[pl.BlockSpec(memory_space=pltpu.VMEM)] * 4,
        out_specs=pl.BlockSpec(memory_space=pltpu.VMEM),
        scratch_shapes=[
            pltpu.VMEM((3072, 128), jnp.float32),
            pltpu.VMEM((256, 2048), jnp.float32),
        ],
    )(message.astype(jnp.float32).reshape(3328, 128), forward, inverse, spread)


def outgoing_kernel(live_ref, field_ref, operator_ref, tiles_ref, operator_out_ref):
    row = lax.broadcasted_iota(jnp.int32, (128, 128), 0)
    for line in range(2):
        for half in range(2):
            live = row + 128 * half < live_ref[line]
            for t in range(3):
                block = jnp.concatenate(
                    [
                        field_ref[pl.ds(384 * c + 128 * t + 2 * half + line, 32, stride=4), :]
                        for c in range(4)
                    ],
                    0,
                )
                block = jnp.where(live, block.T, jnp.float32(0.0))
                tiles_ref[16 * half : 16 * half + 16, 3 * line + t] = block.reshape(16, 8, 128)
    for half in range(2):
        high = []
        low = []
        for line in range(2):
            block = operator_ref[pl.ds(2 * half + line, 32, stride=4), :]
            rounded = block.astype(jnp.bfloat16).astype(jnp.float32)
            rest = ((block - rounded) * LOW_SCALE).astype(jnp.bfloat16).astype(jnp.float32)
            high.append(rounded)
            low.append(rest)
        block = jnp.concatenate(high + low, 0).T
        operator_out_ref[16 * half : 16 * half + 16, 0] = block.reshape(16, 8, 128)


def outgoing(field, live_count, decomposer):
    rows = field.reshape(2, 4, 96, 2, 2, 128).transpose(0, 1, 2, 4, 3, 5).reshape(3072, 128)
    operator_rows = decomposer.reshape(32, 2, 2, 128).transpose(0, 2, 1, 3).reshape(128, 128)
    tiles, operators = pl.pallas_call(
        outgoing_kernel,
        grid=(2,),
        out_shape=(
            jax.ShapeDtypeStruct((32, 12, 8, 128), jnp.float32),
            jax.ShapeDtypeStruct((32, 1, 8, 128), jnp.float32),
        ),
        in_specs=[
            pl.BlockSpec(memory_space=pltpu.SMEM),
            pl.BlockSpec((1536, 128), lambda part: (part, 0)),
            pl.BlockSpec((128, 128), lambda part: (0, 0)),
        ],
        out_specs=(
            pl.BlockSpec((32, 6, 8, 128), lambda part: (0, part, 0, 0)),
            pl.BlockSpec((32, 1, 8, 128), lambda part: (0, 0, 0, 0)),
        ),
    )(live_count, rows, operator_rows)
    return jnp.concatenate([tiles, operators], 1).astype(jnp.float16)


def panel_blocks(reflection):
    panel = reflection[0].reshape(4, 4, 2, 32, 1024).transpose(2, 1, 0, 3, 4).reshape(1024, 1024)
    taken = jnp.arange(1024, dtype=jnp.int32)
    part, line, device, receiver = taken // 512, taken // 256 % 2, taken // 32 % 8, taken % 32
    place = ((device * 2 + part) * 2 + line) * 32 + receiver
    moved = (place[:, None] == taken[None, :]).astype(jnp.bfloat16)
    panel = jnp.dot(panel, moved, preferred_element_type=jnp.float32).astype(jnp.bfloat16)
    return panel.reshape(1024, 8, 128).transpose(1, 0, 2)


def exchanged(blocks):
    rank = lax.axis_index(PLANE)
    received = [lax.dynamic_index_in_dim(blocks, rank, keepdims=False)]
    for distance in range(1, 8):
        block = lax.dynamic_index_in_dim(blocks, rank ^ distance, keepdims=False)
        pairs = [(i, i ^ distance) for i in range(8)]
        received.append(lax.ppermute(block, PLANE, pairs))
    return received


def panel_halves(received):
    rank = lax.axis_index(PLANE)
    core = lax.axis_index("line_2")
    stack = jnp.stack(received)
    halves = []
    for half in (1 - core, core):
        rows = [
            lax.dynamic_slice(stack, (rank ^ source, half * 512, 0), (1, 512, 128))[0]
            for source in range(8)
        ]
        halves.append(jnp.concatenate(rows, 1))
    return halves


def summed(blocks, axis, scale):
    count = lax.axis_size(axis)
    blocks = (blocks * scale).astype(jnp.float16).reshape(count, -1, blocks.shape[-1])
    blocks = lax.all_to_all(blocks, axis, 0, 0, tiled=True)
    return blocks.astype(jnp.float32).sum(axis=0) * (1.0 / scale)


def over_copies(shard, axis):
    count = lax.axis_size(axis)
    shards = jnp.broadcast_to(shard[None], (count, *shard.shape))
    return lax.all_to_all(shards, axis, 0, 0, tiled=True).sum(axis=0)


def on_device(field, live_count, line_owner, decomposer, reflection, direct_wave):
    forward, inverse = transform_tables(line_owner)
    total_freqs = lax.axis_size("freq")
    weight = 2.0 * (lax.axis_index("freq") + 1).astype(jnp.float32) / (total_freqs * (total_freqs + 1))
    weight = jnp.full((32,), weight)
    message = outgoing(field, live_count, decomposer)
    message, reflection, weight = lax.optimization_barrier((message, reflection, weight))
    message = lax.all_to_all(message, RECEIVER, 0, 0, tiled=True)
    received = exchanged(panel_blocks(reflection))
    wave = middle(message, forward, inverse, spread_table())
    wave = lax.all_to_all(wave, "line_0", 0, 0, tiled=True)
    other_panel, own_panel = panel_halves(received)
    wave = wave.reshape(4, 8, 2, 2, 3, 8, 128).transpose(3, 1, 2, 0, 5, 4, 6).reshape(2, 8, 64, 384)
    stacked = jnp.stack(
        [jnp.concatenate([wave[0], wave[1]], 2), jnp.concatenate([-wave[1], wave[0]], 2)], 1
    ).reshape(1024, 768)
    sent = jnp.dot(other_panel, stacked, preferred_element_type=jnp.float32).astype(jnp.float16)
    sent = lax.ppermute(sent, "line_2", [(0, 1), (1, 0)])
    product = jnp.dot(own_panel, stacked, preferred_element_type=jnp.float32)
    product = product + sent.astype(jnp.float32)
    product = summed(product, "line_1", 0.5)
    product = summed(product, "line_0", 0.125)
    reflected = product.reshape(32, 2, 3, 4, 32).transpose(0, 1, 3, 2, 4).reshape(32, 1, 2, 384)
    focusing = direct_wave - reflected
    partial_value = jnp.sum(reflected * reflected, axis=(1, 2, 3)) * weight
    focusing, partial_value = lax.optimization_barrier((focusing, partial_value))
    energy_sum = over_copies(partial_value, "freq")
    trace_energy = jnp.sqrt(energy_sum / 768 + 1e-06)
    return (focusing, trace_energy)


def solution(mesh):
    finer = Mesh(
        mesh.devices.reshape(mesh.shape["freq"], 4, 4, 2), ("freq", "line_0", "line_1", "line_2")
    )
    in_specs = (
        P("freq", None, None, None, LINE, None),
        P(LINE),
        P(),
        P("freq", None, None, None, LINE, None),
        P("freq", None, None, LINE),
        P(LINE, "freq", None, None),
    )
    out_specs = (P(LINE, "freq", None, None), P(LINE))
    return jax.shard_map(
        on_device, mesh=finer, in_specs=in_specs, out_specs=out_specs, check_vma=False
    )
```

```python
import math

import jax
import jax.numpy as jnp
from jax import lax
from jax.experimental import pallas as pl
from jax.experimental.pallas import tpu as pltpu
from jax.sharding import Mesh
from jax.sharding import PartitionSpec as P

LINE = ("line_0", "line_1", "line_2")
RECEIVER = ("line_1", "line_2", "line_0")
PLANE = ("line_1", "line_2")
LOW_SCALE = 256.0


def by_receiver_owner(values):
    return values.reshape(4, 4, 2, 2).transpose(3, 1, 2, 0).reshape(64)


def by_line_owner(values):
    return values.reshape(32, 2).T.reshape(64)


def phases(wavenum, owner):
    products = wavenum[:, None] * owner[None, :] % 64
    angles = products.astype(jnp.float32) * (2.0 * math.pi / 64)
    return (jnp.cos(angles), jnp.sin(angles))


def in_two_terms(table):
    high = lax.reduce_precision(table, 8, 7)
    low = lax.reduce_precision(table - high, 8, 7)
    high = high.astype(jnp.bfloat16)
    low = low.astype(jnp.bfloat16)
    return jnp.concatenate(
        [jnp.concatenate([high, high], 1), jnp.concatenate([low, low], 1)], 0
    )


def transform_tables(line_owner):
    wavenum = by_receiver_owner(jnp.arange(64, dtype=jnp.int32))
    cosine, sine = phases(wavenum, by_receiver_owner(line_owner))
    forward = jnp.stack([jnp.stack([cosine, sine]), jnp.stack([-sine, cosine])])
    forward = forward.transpose(0, 2, 1, 3).reshape(128, 128)
    cosine, sine = phases(wavenum, by_line_owner(line_owner))
    inverse = jnp.stack([jnp.stack([cosine.T, -sine.T]), jnp.stack([sine.T, cosine.T])]) / 64
    inverse = inverse.reshape(2, 2, 2, 32, 64).transpose(2, 0, 3, 1, 4).reshape(128, 128)
    return in_two_terms(forward), in_two_terms(inverse)


def spread_table():
    row = jnp.arange(128, dtype=jnp.int32)[:, None]
    column = jnp.arange(2048, dtype=jnp.int32)[None, :]
    low, line, part, target, source = row // 64, row // 32 % 2, row // 16 % 2, row // 4 % 4, row % 4
    shift, goal = column // 128 % 4, column // 32 % 4
    found = (line == column // 1024) & (part == column // 512 % 2) & (target == goal)
    found = found & (source == (goal - shift) % 4)
    return jnp.where(found, jnp.where(low == 1, 1.0 / LOW_SCALE, 1.0), 0.0).astype(jnp.bfloat16)


def middle_kernel(message_ref, forward_ref, inverse_ref, spread_ref, out_ref, wave_ref, spread_out_ref):
    forward = forward_ref[...]
    inverse = inverse_ref[...]
    operators = jnp.concatenate(
        [message_ref[pl.ds(96 + r, 32, stride=104), :] for r in range(8)], 0
    ).astype(jnp.bfloat16)
    spread_out_ref[...] = jnp.dot(operators, spread_ref[...], preferred_element_type=jnp.float32)

    def transform(table, value):
        high = value.astype(jnp.bfloat16)
        low = (value - high.astype(jnp.float32)).astype(jnp.bfloat16)
        both = jnp.dot(
            table, jnp.concatenate([high, low], 0), preferred_element_type=jnp.float32
        )
        return both[:128] + both[128:]

    for r in range(8):
        tiles = [
            jnp.concatenate(
                [message_ref[pl.ds((g * 3 + t) * 8 + r, 32, stride=104), :] for g in range(4)], 0
            )
            for t in range(3)
        ]
        spectrum = transform(forward, jnp.concatenate(tiles, 1))
        decomposed = []
        for t in range(3):
            field_real = spectrum[:64, 128 * t : 128 * t + 128]
            field_imag = spectrum[64:, 128 * t : 128 * t + 128]
            real_sum = None
            imag_sum = None
            for shift in range(4):
                weight_real, weight_imag = [
                    jnp.concatenate(
                        [
                            spread_out_ref[
                                32 * r : 32 * r + 32, pl.ds(1024 * line + 512 * part + 128 * shift, 128)
                            ]
                            for line in range(2)
                        ],
                        0,
                    )
                    for part in range(2)
                ]
                moved_real = pltpu.roll(field_real, 32 * shift, 1) if shift else field_real
                moved_imag = pltpu.roll(field_imag, 32 * shift, 1) if shift else field_imag
                term_real = weight_real * moved_real - weight_imag * moved_imag
                term_imag = weight_real * moved_imag + weight_imag * moved_real
                real_sum = term_real if real_sum is None else real_sum + term_real
                imag_sum = term_imag if imag_sum is None else imag_sum + term_imag
            decomposed.append(jnp.concatenate([real_sum, imag_sum], 0))
        wave = transform(inverse, jnp.concatenate(decomposed, 1))
        for g in range(4):
            for t in range(3):
                wave_ref[pl.ds((g * 3 + t) * 8 + r, 32, stride=96), :] = wave[
                    32 * g : 32 * g + 32, 128 * t : 128 * t + 128
                ]
    out_ref[...] = wave_ref[...].reshape(32, 12, 8, 128).astype(jnp.bfloat16)


def middle(message, forward, inverse, spread):
    return pl.pallas_call(
        middle_kernel,
        out_shape=pltpu.VMEM((32, 12, 8, 128), jnp.bfloat16),
        in_specs=[pl.BlockSpec(memory_space=pltpu.VMEM)] * 4,
        out_specs=pl.BlockSpec(memory_space=pltpu.VMEM),
        scratch_shapes=[
            pltpu.VMEM((3072, 128), jnp.float32),
            pltpu.VMEM((256, 2048), jnp.float32),
        ],
    )(
        pltpu.with_memory_space_constraint(message.astype(jnp.float32).reshape(3328, 128), pltpu.VMEM),
        *[pltpu.with_memory_space_constraint(table, pltpu.VMEM) for table in (forward, inverse, spread)],
    )


def outgoing_kernel(live_ref, field_ref, operator_ref, out_ref):
    part = pl.program_id(0)
    row = lax.broadcasted_iota(jnp.int32, (128, 128), 0)
    for line in range(2):
        for half in range(2):
            live = row + 128 * half < live_ref[line]
            for t in range(3):
                block = jnp.concatenate(
                    [
                        field_ref[pl.ds(384 * c + 128 * t + 2 * half + line, 32, stride=4), :]
                        for c in range(4)
                    ],
                    0,
                )
                block = jnp.where(live, block.T, jnp.float32(0.0))
                out_ref[16 * half : 16 * half + 16, 6 * part + 3 * line + t] = block.reshape(16, 8, 128)
    for half in range(2):
        high = []
        low = []
        for line in range(2):
            block = operator_ref[pl.ds(2 * half + line, 32, stride=4), :]
            rounded = block.astype(jnp.bfloat16).astype(jnp.float32)
            rest = ((block - rounded) * LOW_SCALE).astype(jnp.bfloat16).astype(jnp.float32)
            high.append(rounded)
            low.append(rest)
        block = jnp.concatenate(high + low, 0).T
        out_ref[16 * half : 16 * half + 16, 12] = block.reshape(16, 8, 128)


def outgoing(field, live_count, decomposer):
    rows = field.reshape(2, 4, 96, 2, 2, 128).transpose(0, 1, 2, 4, 3, 5).reshape(3072, 128)
    operator_rows = decomposer.reshape(32, 2, 2, 128).transpose(0, 2, 1, 3).reshape(128, 128)
    tiles = pl.pallas_call(
        outgoing_kernel,
        grid=(2,),
        out_shape=pltpu.VMEM((32, 13, 8, 128), jnp.float32),
        in_specs=[
            pl.BlockSpec(memory_space=pltpu.SMEM),
            pl.BlockSpec((1536, 128), lambda part: (part, 0)),
            pl.BlockSpec((128, 128), lambda part: (0, 0)),
        ],
        out_specs=pl.BlockSpec(memory_space=pltpu.VMEM),
    )(live_count, rows, operator_rows)
    return tiles.astype(jnp.float16)


def panel_blocks(reflection):
    panel = reflection[0].reshape(4, 4, 2, 32, 1024).transpose(2, 1, 0, 3, 4).reshape(1024, 1024)
    taken = jnp.arange(1024, dtype=jnp.int32)
    part, line, device, receiver = taken // 512, taken // 256 % 2, taken // 32 % 8, taken % 32
    place = ((device * 2 + part) * 2 + line) * 32 + receiver
    moved = (place[:, None] == taken[None, :]).astype(jnp.bfloat16)
    panel = jnp.dot(panel, moved, preferred_element_type=jnp.float32).astype(jnp.bfloat16)
    return panel.reshape(1024, 8, 128).transpose(1, 0, 2)


def exchanged(blocks):
    rank = lax.axis_index(PLANE)
    received = [lax.dynamic_index_in_dim(blocks, rank, keepdims=False)]
    for distance in range(1, 8):
        block = lax.dynamic_index_in_dim(blocks, rank ^ distance, keepdims=False)
        pairs = [(i, i ^ distance) for i in range(8)]
        received.append(lax.ppermute(block, PLANE, pairs))
    return received


def panel_halves(received):
    rank = lax.axis_index(PLANE)
    core = lax.axis_index("line_2")
    stack = jnp.stack(received)
    halves = []
    for half in (1 - core, core):
        rows = [
            lax.dynamic_slice(stack, (rank ^ source, half * 512, 0), (1, 512, 128))[0]
            for source in range(8)
        ]
        halves.append(jnp.concatenate(rows, 1))
    return halves


def summed(blocks, axis, scale):
    count = lax.axis_size(axis)
    blocks = (blocks * scale).astype(jnp.float16).reshape(count, -1, blocks.shape[-1])
    blocks = lax.all_to_all(blocks, axis, 0, 0, tiled=True)
    return blocks.astype(jnp.float32).sum(axis=0) * (1.0 / scale)


def over_copies(shard, axis):
    count = lax.axis_size(axis)
    shards = jnp.broadcast_to(shard[None], (count, *shard.shape))
    return lax.all_to_all(shards, axis, 0, 0, tiled=True).sum(axis=0)


def on_device(field, live_count, line_owner, decomposer, reflection, direct_wave):
    forward, inverse = transform_tables(line_owner)
    total_freqs = lax.axis_size("freq")
    weight = 2.0 * (lax.axis_index("freq") + 1).astype(jnp.float32) / (total_freqs * (total_freqs + 1))
    weight = jnp.full((32,), weight)
    message = outgoing(field, live_count, decomposer)
    message, reflection, weight = lax.optimization_barrier((message, reflection, weight))
    message = lax.all_to_all(message, RECEIVER, 0, 0, tiled=True)
    received = exchanged(panel_blocks(reflection))
    wave = middle(message, forward, inverse, spread_table())
    wave = lax.all_to_all(wave, "line_0", 0, 0, tiled=True)
    other_panel, own_panel = panel_halves(received)
    wave = wave.reshape(4, 8, 2, 2, 3, 8, 128).transpose(3, 1, 2, 0, 5, 4, 6).reshape(2, 8, 64, 384)
    stacked = jnp.stack(
        [jnp.concatenate([wave[0], wave[1]], 2), jnp.concatenate([-wave[1], wave[0]], 2)], 1
    ).reshape(1024, 768)
    sent = jnp.dot(other_panel, stacked, preferred_element_type=jnp.float32).astype(jnp.float16)
    sent = lax.ppermute(sent, "line_2", [(0, 1), (1, 0)])
    product = lax.optimization_barrier(
        jnp.dot(own_panel, stacked, preferred_element_type=jnp.float32)
    )
    product = product + sent.astype(jnp.float32)
    product = summed(product, "line_1", 0.5)
    product = summed(product, "line_0", 0.125)
    reflected = product.reshape(32, 2, 3, 4, 32).transpose(0, 1, 3, 2, 4).reshape(32, 1, 2, 384)
    partial_value = jnp.sum(product * product, axis=1) * weight
    reflected, partial_value = lax.optimization_barrier((reflected, partial_value))
    energy_sum = over_copies(partial_value, "freq")
    reflected, energy_sum = lax.optimization_barrier((reflected, energy_sum))
    focusing = direct_wave - reflected
    trace_energy = jnp.sqrt(energy_sum / 768 + 1e-06)
    return (focusing, trace_energy)


def solution(mesh):
    finer = Mesh(
        mesh.devices.reshape(mesh.shape["freq"], 4, 4, 2), ("freq", "line_0", "line_1", "line_2")
    )
    in_specs = (
        P("freq", None, None, None, LINE, None),
        P(LINE),
        P(),
        P("freq", None, None, None, LINE, None),
        P("freq", None, None, LINE),
        P(LINE, "freq", None, None),
    )
    out_specs = (P(LINE, "freq", None, None), P(LINE))
    return jax.shard_map(
        on_device, mesh=finer, in_specs=in_specs, out_specs=out_specs, check_vma=False
    )
```

```python
import math

import jax
import jax.numpy as jnp
from jax import lax
from jax.experimental import pallas as pl
from jax.experimental.pallas import tpu as pltpu
from jax.sharding import Mesh
from jax.sharding import PartitionSpec as P

LINE = ("line_0", "line_1", "line_2")
RECEIVER = ("line_1", "line_2", "line_0")
PLANE = ("line_1", "line_2")


def by_receiver_owner(values):
    return values.reshape(4, 4, 2, 2).transpose(3, 1, 2, 0).reshape(64)


def by_line_owner(values):
    return values.reshape(32, 2).T.reshape(64)


def phases(wavenum, owner):
    products = wavenum[:, None] * owner[None, :] % 64
    angles = products.astype(jnp.float32) * (2.0 * math.pi / 64)
    return (jnp.cos(angles), jnp.sin(angles))


def in_two_terms(table):
    high = lax.reduce_precision(table, 8, 7)
    low = lax.reduce_precision(table - high, 8, 7)
    high = high.astype(jnp.bfloat16)
    low = low.astype(jnp.bfloat16)
    return jnp.concatenate(
        [jnp.concatenate([high, high], 1), jnp.concatenate([low, low], 1)], 0
    )


def transform_tables(line_owner):
    wavenum = by_receiver_owner(jnp.arange(64, dtype=jnp.int32))
    cosine, sine = phases(wavenum, by_receiver_owner(line_owner))
    forward = jnp.stack([jnp.stack([cosine, sine]), jnp.stack([-sine, cosine])])
    forward = forward.transpose(0, 2, 1, 3).reshape(128, 128)
    cosine, sine = phases(wavenum, by_line_owner(line_owner))
    inverse = jnp.stack([jnp.stack([cosine.T, -sine.T]), jnp.stack([sine.T, cosine.T])]) / 64
    inverse = inverse.reshape(2, 2, 2, 32, 64).transpose(2, 0, 3, 1, 4).reshape(128, 128)
    return in_two_terms(forward), in_two_terms(inverse)


def spread_table():
    row = jnp.arange(128, dtype=jnp.int32)[:, None]
    column = jnp.arange(2048, dtype=jnp.int32)[None, :]
    line, part, target, source = row // 32 % 2, row // 16 % 2, row // 4 % 4, row % 4
    shift, goal = column // 128 % 4, column // 32 % 4
    found = (line == column // 1024) & (part == column // 512 % 2) & (target == goal)
    found = found & (source == (goal - shift) % 4)
    return found.astype(jnp.bfloat16)


def middle_kernel(message_ref, forward_ref, inverse_ref, spread_ref, out_ref, wave_ref, spread_out_ref):
    forward = forward_ref[...]
    inverse = inverse_ref[...]
    lane = lax.broadcasted_iota(jnp.int32, (32, 128), 1)
    early = []
    late = []
    for r in range(4):
        block = message_ref[pl.ds(96 + r, 32, stride=100), :]
        high = block.astype(jnp.bfloat16).astype(jnp.float32)
        low = block - high
        early.append(jnp.where(lane < 64, high, pltpu.roll(low, 64, 1)))
        late.append(jnp.where(lane < 64, pltpu.roll(high, 64, 1), low))
    operators = jnp.concatenate(early + late, 0).astype(jnp.bfloat16)
    spread_out_ref[...] = jnp.dot(operators, spread_ref[...], preferred_element_type=jnp.float32)

    def transform(table, value):
        high = value.astype(jnp.bfloat16)
        low = (value - high.astype(jnp.float32)).astype(jnp.bfloat16)
        both = jnp.dot(
            table, jnp.concatenate([high, low], 0), preferred_element_type=jnp.float32
        )
        return both[:128] + both[128:]

    for r in range(8):
        tiles = [
            jnp.concatenate(
                [message_ref[pl.ds((g * 3 + t) * 8 + r, 32, stride=100), :] for g in range(4)], 0
            )
            for t in range(3)
        ]
        spectrum = transform(forward, jnp.concatenate(tiles, 1))
        decomposed = []
        for t in range(3):
            field_real = spectrum[:64, 128 * t : 128 * t + 128]
            field_imag = spectrum[64:, 128 * t : 128 * t + 128]
            real_sum = None
            imag_sum = None
            for shift in range(4):
                weight_real, weight_imag = [
                    jnp.concatenate(
                        [
                            spread_out_ref[
                                32 * r : 32 * r + 32, pl.ds(1024 * line + 512 * part + 128 * shift, 128)
                            ]
                            for line in range(2)
                        ],
                        0,
                    )
                    for part in range(2)
                ]
                moved_real = pltpu.roll(field_real, 32 * shift, 1) if shift else field_real
                moved_imag = pltpu.roll(field_imag, 32 * shift, 1) if shift else field_imag
                term_real = weight_real * moved_real - weight_imag * moved_imag
                term_imag = weight_real * moved_imag + weight_imag * moved_real
                real_sum = term_real if real_sum is None else real_sum + term_real
                imag_sum = term_imag if imag_sum is None else imag_sum + term_imag
            decomposed.append(jnp.concatenate([real_sum, imag_sum], 0))
        wave = transform(inverse, jnp.concatenate(decomposed, 1))
        for g in range(4):
            for t in range(3):
                wave_ref[pl.ds((g * 3 + t) * 8 + r, 32, stride=96), :] = wave[
                    32 * g : 32 * g + 32, 128 * t : 128 * t + 128
                ]
    out_ref[...] = wave_ref[...].reshape(32, 12, 8, 128).astype(jnp.bfloat16)


def middle(message, forward, inverse, spread):
    return pl.pallas_call(
        middle_kernel,
        out_shape=pltpu.VMEM((32, 12, 8, 128), jnp.bfloat16),
        in_specs=[pl.BlockSpec(memory_space=pltpu.VMEM)] * 4,
        out_specs=pl.BlockSpec(memory_space=pltpu.VMEM),
        scratch_shapes=[
            pltpu.VMEM((3072, 128), jnp.float32),
            pltpu.VMEM((256, 2048), jnp.float32),
        ],
    )(
        pltpu.with_memory_space_constraint(message.astype(jnp.float32).reshape(3200, 128), pltpu.VMEM),
        *[pltpu.with_memory_space_constraint(table, pltpu.VMEM) for table in (forward, inverse, spread)],
    )


def outgoing_kernel(live_ref, field_ref, operator_ref, out_ref):
    row = lax.broadcasted_iota(jnp.int32, (128, 128), 0)
    lane = lax.broadcasted_iota(jnp.int32, (128, 128), 1)

    def put_field(part):
        for line in range(2):
            for half in range(2):
                live = row + 128 * half < live_ref[line]
                for t in range(3):
                    block = jnp.concatenate(
                        [
                            field_ref[pl.ds(384 * c + 128 * t + 2 * half + line, 32, stride=4), :]
                            for c in range(4)
                        ],
                        0,
                    )
                    block = jnp.where(live, block.T, jnp.float32(0.0))
                    for device in range(16):
                        place = 100 * (16 * half + device) + 48 * part + 24 * line + 8 * t
                        out_ref[place : place + 8, :] = block[8 * device : 8 * device + 8]

    def put_operators():
        for half in range(2):
            lines = [operator_ref[pl.ds(2 * half + line, 32, stride=4), :] for line in range(2)]
            block = jnp.concatenate(lines + lines, 0).T
            block = jnp.where(lane < 64, block, pltpu.roll(block, 124, 0))
            for device in range(16):
                place = 100 * (16 * half + device) + 96
                out_ref[place : place + 4, :] = block[8 * device : 8 * device + 4]

    @pl.when(pl.program_id(0) == 0)
    def _():
        put_field(0)
        put_operators()

    @pl.when(pl.program_id(0) == 1)
    def _():
        put_field(1)


def outgoing(field, live_count, decomposer):
    rows = field.reshape(2, 4, 96, 2, 2, 128).transpose(0, 1, 2, 4, 3, 5).reshape(3072, 128)
    operator_rows = decomposer.reshape(32, 2, 2, 128).transpose(0, 2, 1, 3).reshape(128, 128)
    tiles = pl.pallas_call(
        outgoing_kernel,
        grid=(2,),
        out_shape=pltpu.VMEM((3200, 128), jnp.float32),
        in_specs=[
            pl.BlockSpec(memory_space=pltpu.SMEM),
            pl.BlockSpec((1536, 128), lambda part: (part, 0)),
            pl.BlockSpec((128, 128), lambda part: (0, 0)),
        ],
        out_specs=pl.BlockSpec(memory_space=pltpu.VMEM),
    )(live_count, rows, operator_rows)
    return tiles.reshape(32, 25, 4, 128).astype(jnp.float16)


def panel_blocks(reflection):
    panel = reflection[0].reshape(4, 4, 2, 32, 1024).transpose(2, 1, 0, 3, 4).reshape(1024, 1024)
    taken = jnp.arange(1024, dtype=jnp.int32)
    part, line, device, receiver = taken // 512, taken // 256 % 2, taken // 32 % 8, taken % 32
    place = ((device * 2 + part) * 2 + line) * 32 + receiver
    moved = (place[:, None] == taken[None, :]).astype(jnp.bfloat16)
    panel = jnp.dot(panel, moved, preferred_element_type=jnp.float32).astype(jnp.bfloat16)
    return panel.reshape(1024, 8, 128).transpose(1, 0, 2)


def exchanged(blocks):
    rank = lax.axis_index(PLANE)
    received = [lax.dynamic_index_in_dim(blocks, rank, keepdims=False)]
    for distance in range(1, 8):
        block = lax.dynamic_index_in_dim(blocks, rank ^ distance, keepdims=False)
        pairs = [(i, i ^ distance) for i in range(8)]
        received.append(lax.ppermute(block, PLANE, pairs))
    return received


def panel_halves(received):
    rank = lax.axis_index(PLANE)
    core = lax.axis_index("line_2")
    stack = jnp.stack(received)
    halves = []
    for half in (1 - core, core):
        rows = [
            lax.dynamic_slice(stack, (rank ^ source, half * 512, 0), (1, 512, 128))[0]
            for source in range(8)
        ]
        halves.append(jnp.concatenate(rows, 1))
    return halves


def summed(blocks, axis, scale):
    count = lax.axis_size(axis)
    blocks = (blocks * scale).astype(jnp.float16).reshape(count, -1, blocks.shape[-1])
    blocks = lax.all_to_all(blocks, axis, 0, 0, tiled=True)
    return blocks.astype(jnp.float32).sum(axis=0) * (1.0 / scale)


def over_copies(shard, axis):
    count = lax.axis_size(axis)
    shards = jnp.broadcast_to(shard[None], (count, *shard.shape))
    return lax.all_to_all(shards, axis, 0, 0, tiled=True).sum(axis=0)


def on_device(field, live_count, line_owner, decomposer, reflection, direct_wave):
    forward, inverse = transform_tables(line_owner)
    total_freqs = lax.axis_size("freq")
    weight = 2.0 * (lax.axis_index("freq") + 1).astype(jnp.float32) / (total_freqs * (total_freqs + 1))
    weight = jnp.full((32,), weight)
    message = outgoing(field, live_count, decomposer)
    message, reflection, weight = lax.optimization_barrier((message, reflection, weight))
    message = lax.all_to_all(message, RECEIVER, 0, 0, tiled=True)
    received = exchanged(panel_blocks(reflection))
    wave = middle(message, forward, inverse, spread_table())
    wave = lax.all_to_all(wave, "line_0", 0, 0, tiled=True)
    other_panel, own_panel = panel_halves(received)
    wave = wave.reshape(4, 8, 2, 2, 3, 8, 128).transpose(3, 1, 2, 0, 5, 4, 6).reshape(2, 8, 64, 384)
    stacked = jnp.stack(
        [jnp.concatenate([wave[0], wave[1]], 2), jnp.concatenate([-wave[1], wave[0]], 2)], 1
    ).reshape(1024, 768)
    sent = jnp.dot(other_panel, stacked, preferred_element_type=jnp.float32).astype(jnp.float16)
    sent = lax.ppermute(sent, "line_2", [(0, 1), (1, 0)])
    product = lax.optimization_barrier(
        jnp.dot(own_panel, stacked, preferred_element_type=jnp.float32)
    )
    product = product + sent.astype(jnp.float32)
    product = summed(product, "line_1", 0.5)
    product = summed(product, "line_0", 0.125)
    reflected = product.reshape(32, 2, 3, 4, 32).transpose(0, 1, 3, 2, 4).reshape(32, 1, 2, 384)
    partial_value = jnp.sum(product * product, axis=1) * weight
    reflected, partial_value = lax.optimization_barrier((reflected, partial_value))
    energy_sum = over_copies(partial_value, "freq")
    reflected, energy_sum = lax.optimization_barrier((reflected, energy_sum))
    focusing = direct_wave - reflected
    trace_energy = jnp.sqrt(energy_sum / 768 + 1e-06)
    return (focusing, trace_energy)


def solution(mesh):
    finer = Mesh(
        mesh.devices.reshape(mesh.shape["freq"], 4, 4, 2), ("freq", "line_0", "line_1", "line_2")
    )
    in_specs = (
        P("freq", None, None, None, LINE, None),
        P(LINE),
        P(),
        P("freq", None, None, None, LINE, None),
        P("freq", None, None, LINE),
        P(LINE, "freq", None, None),
    )
    out_specs = (P(LINE, "freq", None, None), P(LINE))
    return jax.shard_map(
        on_device, mesh=finer, in_specs=in_specs, out_specs=out_specs, check_vma=False
    )
```

```python
import math

import jax
import jax.numpy as jnp
from jax import lax
from jax.experimental import pallas as pl
from jax.experimental.pallas import tpu as pltpu
from jax.sharding import Mesh
from jax.sharding import PartitionSpec as P

LINE = ("line_0", "line_1", "line_2")
RECEIVER = ("line_1", "line_2", "line_0")
PLANE = ("line_1", "line_2")


def by_receiver_owner(values):
    return values.reshape(4, 4, 2, 2).transpose(3, 1, 2, 0).reshape(64)


def by_line_owner(values):
    return values.reshape(32, 2).T.reshape(64)


def phases(wavenum, owner):
    products = wavenum[:, None] * owner[None, :] % 64
    angles = products.astype(jnp.float32) * (2.0 * math.pi / 64)
    return (jnp.cos(angles), jnp.sin(angles))


def in_two_terms(table):
    high = lax.reduce_precision(table, 8, 7)
    low = lax.reduce_precision(table - high, 8, 7)
    high = high.astype(jnp.bfloat16)
    low = low.astype(jnp.bfloat16)
    return jnp.concatenate(
        [jnp.concatenate([high, high], 1), jnp.concatenate([low, low], 1)], 0
    )


def transform_tables(line_owner):
    wavenum = by_receiver_owner(jnp.arange(64, dtype=jnp.int32))
    cosine, sine = phases(wavenum, by_receiver_owner(line_owner))
    forward = jnp.stack([jnp.stack([cosine, sine]), jnp.stack([-sine, cosine])])
    forward = forward.transpose(0, 2, 1, 3).reshape(128, 128)
    cosine, sine = phases(wavenum, by_line_owner(line_owner))
    inverse = jnp.stack([jnp.stack([cosine.T, -sine.T]), jnp.stack([sine.T, cosine.T])]) / 64
    inverse = inverse.reshape(2, 2, 2, 32, 64).transpose(2, 0, 3, 1, 4).reshape(128, 128)
    return in_two_terms(forward), in_two_terms(inverse)


def spread_table():
    row = jnp.arange(128, dtype=jnp.int32)[:, None]
    column = jnp.arange(2048, dtype=jnp.int32)[None, :]
    line, part, target, source = row // 32 % 2, row // 16 % 2, row // 4 % 4, row % 4
    shift, goal = column // 128 % 4, column // 32 % 4
    found = (line == column // 1024) & (part == column // 512 % 2) & (target == goal)
    found = found & (source == (goal - shift) % 4)
    return found.astype(jnp.bfloat16)


def middle_kernel(message_ref, forward_ref, inverse_ref, spread_ref, out_ref, wave_ref, spread_out_ref, spectrum_ref, decomposed_ref):
    forward = forward_ref[...]
    inverse = inverse_ref[...]
    lane = lax.broadcasted_iota(jnp.int32, (32, 128), 1)
    early = []
    late = []
    for r in range(4):
        block = message_ref[pl.ds(96 + r, 32, stride=100), :]
        high = block.astype(jnp.bfloat16).astype(jnp.float32)
        low = block - high
        early.append(jnp.where(lane < 64, high, pltpu.roll(low, 64, 1)))
        late.append(jnp.where(lane < 64, pltpu.roll(high, 64, 1), low))
    operators = jnp.concatenate(early + late, 0).astype(jnp.bfloat16)
    spread_out_ref[...] = jnp.dot(operators, spread_ref[...], preferred_element_type=jnp.float32)

    def load(r):
        tiles = [
            jnp.concatenate(
                [message_ref[pl.ds((g * 3 + t) * 8 + r, 32, stride=100), :] for g in range(4)], 0
            )
            for t in range(3)
        ]
        value = jnp.concatenate(tiles, 1)
        high = value.astype(jnp.bfloat16)
        low = (value - high.astype(jnp.float32)).astype(jnp.bfloat16)
        both = jnp.dot(
            forward, jnp.concatenate([high, low], 0), preferred_element_type=jnp.float32
        )
        spectrum_ref[r % 2] = both[:128] + both[128:]

    def decompose(r):
        for t in range(3):
            at = pl.ds(128 * t, 128)
            for line in range(2):
                rows = pl.ds(32 * line, 32)
                imag_rows = pl.ds(64 + 32 * line, 32)
                field_real = spectrum_ref[r % 2, rows, at]
                field_imag = spectrum_ref[r % 2, imag_rows, at]
                real_sum = None
                imag_sum = None
                for shift in range(4):
                    weight_real, weight_imag = [
                        spread_out_ref[
                            32 * r : 32 * r + 32, pl.ds(1024 * line + 512 * part + 128 * shift, 128)
                        ]
                        for part in range(2)
                    ]
                    moved_real = pltpu.roll(field_real, 32 * shift, 1) if shift else field_real
                    moved_imag = pltpu.roll(field_imag, 32 * shift, 1) if shift else field_imag
                    term_real = weight_real * moved_real - weight_imag * moved_imag
                    term_imag = weight_real * moved_imag + weight_imag * moved_real
                    real_sum = term_real if real_sum is None else real_sum + term_real
                    imag_sum = term_imag if imag_sum is None else imag_sum + term_imag
                for value, first in ((real_sum, 0), (imag_sum, 64)):
                    high = value.astype(jnp.bfloat16)
                    low = (value - high.astype(jnp.float32)).astype(jnp.bfloat16)
                    decomposed_ref[r % 2, pl.ds(first + 32 * line, 32), at] = high
                    decomposed_ref[r % 2, pl.ds(128 + first + 32 * line, 32), at] = low

    def store(r):
        both = jnp.dot(inverse, decomposed_ref[r % 2], preferred_element_type=jnp.float32)
        wave = both[:128] + both[128:]
        for g in range(4):
            for t in range(3):
                wave_ref[pl.ds((g * 3 + t) * 8 + r, 32, stride=96), :] = wave[
                    32 * g : 32 * g + 32, 128 * t : 128 * t + 128
                ]

    load(0)
    for r in range(8):
        if r < 7:
            load(r + 1)
        decompose(r)
        store(r)
    out_ref[...] = wave_ref[...].reshape(32, 12, 8, 128).astype(jnp.bfloat16)


def middle(message, forward, inverse, spread):
    return pl.pallas_call(
        middle_kernel,
        out_shape=pltpu.VMEM((32, 12, 8, 128), jnp.bfloat16),
        in_specs=[pl.BlockSpec(memory_space=pltpu.VMEM)] * 4,
        out_specs=pl.BlockSpec(memory_space=pltpu.VMEM),
        scratch_shapes=[
            pltpu.VMEM((3072, 128), jnp.float32),
            pltpu.VMEM((256, 2048), jnp.float32),
            pltpu.VMEM((2, 128, 384), jnp.float32),
            pltpu.VMEM((2, 256, 384), jnp.bfloat16),
        ],
    )(
        pltpu.with_memory_space_constraint(message.astype(jnp.float32).reshape(3200, 128), pltpu.VMEM),
        *[pltpu.with_memory_space_constraint(table, pltpu.VMEM) for table in (forward, inverse, spread)],
    )


def outgoing_kernel(live_ref, field_ref, operator_ref, out_ref):
    row = lax.broadcasted_iota(jnp.int32, (128, 128), 0)
    lane = lax.broadcasted_iota(jnp.int32, (128, 128), 1)

    def put_field(part):
        for line in range(2):
            for half in range(2):
                live = row + 128 * half < live_ref[line]
                for t in range(3):
                    block = jnp.concatenate(
                        [
                            field_ref[pl.ds(384 * c + 128 * t + 2 * half + line, 32, stride=4), :]
                            for c in range(4)
                        ],
                        0,
                    )
                    block = jnp.where(live, block.T, jnp.float32(0.0))
                    for device in range(16):
                        place = 100 * (16 * half + device) + 48 * part + 24 * line + 8 * t
                        out_ref[place : place + 8, :] = block[8 * device : 8 * device + 8]

    def put_operators():
        for half in range(2):
            lines = [operator_ref[pl.ds(2 * half + line, 32, stride=4), :] for line in range(2)]
            block = jnp.concatenate(lines + lines, 0).T
            block = jnp.where(lane < 64, block, pltpu.roll(block, 124, 0))
            for device in range(16):
                place = 100 * (16 * half + device) + 96
                out_ref[place : place + 4, :] = block[8 * device : 8 * device + 4]

    @pl.when(pl.program_id(0) == 0)
    def _():
        put_field(0)
        put_operators()

    @pl.when(pl.program_id(0) == 1)
    def _():
        put_field(1)


def outgoing(field, live_count, decomposer):
    rows = field.reshape(2, 4, 96, 2, 2, 128).transpose(0, 1, 2, 4, 3, 5).reshape(3072, 128)
    operator_rows = decomposer.reshape(32, 2, 2, 128).transpose(0, 2, 1, 3).reshape(128, 128)
    tiles = pl.pallas_call(
        outgoing_kernel,
        grid=(2,),
        out_shape=pltpu.VMEM((3200, 128), jnp.float32),
        in_specs=[
            pl.BlockSpec(memory_space=pltpu.SMEM),
            pl.BlockSpec((1536, 128), lambda part: (part, 0)),
            pl.BlockSpec((128, 128), lambda part: (0, 0)),
        ],
        out_specs=pl.BlockSpec(memory_space=pltpu.VMEM),
    )(live_count, rows, operator_rows)
    return tiles.reshape(32, 25, 4, 128).astype(jnp.float16)


def panel_blocks(reflection):
    panel = reflection[0].reshape(4, 4, 2, 32, 1024).transpose(2, 1, 0, 3, 4).reshape(1024, 1024)
    taken = jnp.arange(1024, dtype=jnp.int32)
    part, line, device, receiver = taken // 512, taken // 256 % 2, taken // 32 % 8, taken % 32
    place = ((device * 2 + part) * 2 + line) * 32 + receiver
    moved = (place[:, None] == taken[None, :]).astype(jnp.bfloat16)
    panel = jnp.dot(panel, moved, preferred_element_type=jnp.float32).astype(jnp.bfloat16)
    return panel.reshape(1024, 8, 128).transpose(1, 0, 2)


def exchanged(blocks):
    rank = lax.axis_index(PLANE)
    received = [lax.dynamic_index_in_dim(blocks, rank, keepdims=False)]
    for distance in range(1, 8):
        block = lax.dynamic_index_in_dim(blocks, rank ^ distance, keepdims=False)
        pairs = [(i, i ^ distance) for i in range(8)]
        received.append(lax.ppermute(block, PLANE, pairs))
    return received


def panel_halves(received):
    rank = lax.axis_index(PLANE)
    core = lax.axis_index("line_2")
    stack = jnp.stack(received)
    halves = []
    for half in (1 - core, core):
        rows = [
            lax.dynamic_slice(stack, (rank ^ source, half * 512, 0), (1, 512, 128))[0]
            for source in range(8)
        ]
        halves.append(jnp.concatenate(rows, 1))
    return halves


def summed(blocks, axis, scale):
    count = lax.axis_size(axis)
    blocks = (blocks * scale).astype(jnp.float16).reshape(count, -1, blocks.shape[-1])
    blocks = lax.all_to_all(blocks, axis, 0, 0, tiled=True)
    return blocks.astype(jnp.float32).sum(axis=0) * (1.0 / scale)


def closing_kernel(blocks_ref, direct_ref, weight_ref, focusing_ref, energies_ref):
    lane = lax.broadcasted_iota(jnp.int32, (32, 128), 1)
    energy = jnp.zeros((32, 128), jnp.float32)
    for part in range(2):
        tiles = []
        for t in range(3):
            at = pl.ds(384 * part + 128 * t, 128)
            tile = blocks_ref[0, :, at] + blocks_ref[1, :, at]
            tile = (tile + blocks_ref[2, :, at] + blocks_ref[3, :, at]) * jnp.float32(8.0)
            energy = energy + tile * tile
            tiles.append(tile)
        for t in range(3):
            natural = None
            for place in range(4):
                chunk = 4 * t + place
                source = tiles[chunk % 3]
                shift = 32 * (place - chunk // 3) % 128
                moved = pltpu.roll(source, shift, 1) if shift else source
                natural = moved if natural is None else jnp.where(lane < 32 * place, natural, moved)
            at = pl.ds(128 * t, 128)
            focusing_ref[:, 0, part, at] = direct_ref[:, 0, part, at] - natural
    total = jnp.sum(energy, axis=1, keepdims=True) * weight_ref[...]
    energies_ref[...] = total.T[:16].reshape(16, 1, 32)


def closing(blocks, direct_wave, weight):
    return pl.pallas_call(
        closing_kernel,
        out_shape=(
            jax.ShapeDtypeStruct((32, 1, 2, 384), jnp.float32),
            pltpu.VMEM((16, 1, 32), jnp.float32),
        ),
        in_specs=[pl.BlockSpec(memory_space=pltpu.VMEM)] * 3,
        out_specs=(pl.BlockSpec(memory_space=pltpu.VMEM), pl.BlockSpec(memory_space=pltpu.VMEM)),
    )(
        pltpu.with_memory_space_constraint(blocks.astype(jnp.float32), pltpu.VMEM),
        pltpu.with_memory_space_constraint(direct_wave, pltpu.VMEM),
        pltpu.with_memory_space_constraint(weight, pltpu.VMEM),
    )


def on_device(field, live_count, line_owner, decomposer, reflection, direct_wave):
    forward, inverse = transform_tables(line_owner)
    total_freqs = lax.axis_size("freq")
    weight = 2.0 * (lax.axis_index("freq") + 1).astype(jnp.float32) / (total_freqs * (total_freqs + 1))
    weight = jnp.full((1, 128), weight)
    message = outgoing(field, live_count, decomposer)
    message, reflection, weight = lax.optimization_barrier((message, reflection, weight))
    message = lax.all_to_all(message, RECEIVER, 0, 0, tiled=True)
    received = exchanged(panel_blocks(reflection))
    wave = middle(message, forward, inverse, spread_table())
    wave = lax.all_to_all(wave, "line_0", 0, 0, tiled=True)
    other_panel, own_panel = panel_halves(received)
    wave = wave.reshape(4, 8, 2, 2, 3, 8, 128).transpose(3, 1, 2, 0, 5, 4, 6).reshape(2, 8, 64, 384)
    stacked = jnp.stack(
        [jnp.concatenate([wave[0], wave[1]], 2), jnp.concatenate([-wave[1], wave[0]], 2)], 1
    ).reshape(1024, 768)
    sent = jnp.dot(other_panel, stacked, preferred_element_type=jnp.float32).astype(jnp.float16)
    sent = lax.ppermute(sent, "line_2", [(0, 1), (1, 0)])
    product = lax.optimization_barrier(
        jnp.dot(own_panel, stacked, preferred_element_type=jnp.float32)
    )
    product = product + sent.astype(jnp.float32)
    product = summed(product, "line_1", 0.5)
    blocks = (product * 0.125).astype(jnp.float16).reshape(4, 32, 768)
    blocks = lax.all_to_all(blocks, "line_0", 0, 0, tiled=True)
    focusing, energies = closing(blocks, direct_wave, weight)
    energies = lax.all_to_all(energies, "freq", 0, 0, tiled=True)
    energy_sum = energies.reshape(16, 32).sum(axis=0)
    trace_energy = jnp.sqrt(energy_sum / 768 + 1e-06)
    return (focusing, trace_energy)


def solution(mesh):
    finer = Mesh(
        mesh.devices.reshape(mesh.shape["freq"], 4, 4, 2), ("freq", "line_0", "line_1", "line_2")
    )
    in_specs = (
        P("freq", None, None, None, LINE, None),
        P(LINE),
        P(),
        P("freq", None, None, None, LINE, None),
        P("freq", None, None, LINE),
        P(LINE, "freq", None, None),
    )
    out_specs = (P(LINE, "freq", None, None), P(LINE))
    return jax.shard_map(
        on_device, mesh=finer, in_specs=in_specs, out_specs=out_specs, check_vma=False
    )
```

```python
import math

import jax
import jax.numpy as jnp
from jax import lax
from jax.experimental import pallas as pl
from jax.experimental.pallas import tpu as pltpu
from jax.sharding import Mesh
from jax.sharding import PartitionSpec as P

LINE = ("line_0", "line_1", "line_2")
RECEIVER = ("line_1", "line_2", "line_0")
PLANE = ("line_1", "line_2")


def by_receiver_owner(values):
    return values.reshape(4, 4, 2, 2).transpose(3, 1, 2, 0).reshape(64)


def by_line_owner(values):
    return values.reshape(32, 2).T.reshape(64)


def phases(wavenum, owner):
    products = wavenum[:, None] * owner[None, :] % 64
    angles = products.astype(jnp.float32) * (2.0 * math.pi / 64)
    return (jnp.cos(angles), jnp.sin(angles))


def in_two_terms(table):
    high = lax.reduce_precision(table, 8, 7)
    low = lax.reduce_precision(table - high, 8, 7)
    high = high.astype(jnp.bfloat16)
    low = low.astype(jnp.bfloat16)
    return jnp.concatenate(
        [jnp.concatenate([high, high], 1), jnp.concatenate([low, low], 1)], 0
    )


def transform_tables(line_owner):
    wavenum = by_receiver_owner(jnp.arange(64, dtype=jnp.int32))
    cosine, sine = phases(wavenum, by_receiver_owner(line_owner))
    forward = jnp.stack([jnp.stack([cosine, sine]), jnp.stack([-sine, cosine])])
    forward = forward.transpose(0, 2, 1, 3).reshape(128, 128)
    cosine, sine = phases(wavenum, by_line_owner(line_owner))
    inverse = jnp.stack([jnp.stack([cosine.T, -sine.T]), jnp.stack([sine.T, cosine.T])]) / 64
    inverse = inverse.reshape(2, 2, 2, 32, 64).transpose(2, 0, 3, 1, 4).reshape(128, 128)
    return in_two_terms(forward), in_two_terms(inverse)


def spread_table():
    row = jnp.arange(128, dtype=jnp.int32)[:, None]
    column = jnp.arange(2048, dtype=jnp.int32)[None, :]
    line, part, target, source = row // 32 % 2, row // 16 % 2, row // 4 % 4, row % 4
    shift, goal = column // 128 % 4, column // 32 % 4
    found = (line == column // 1024) & (part == column // 512 % 2) & (target == goal)
    found = found & (source == (goal - shift) % 4)
    return found.astype(jnp.bfloat16)


def middle_kernel(
    message_ref,
    forward_ref,
    inverse_ref,
    spread_ref,
    out_ref,
    wave_ref,
    spread_out_ref,
    spectrum_ref,
    decomposed_ref,
    ready_ref,
    sent,
):
    forward = forward_ref[...]
    inverse = inverse_ref[...]
    lane = lax.broadcasted_iota(jnp.int32, (32, 128), 1)
    early = []
    late = []
    for r in range(4):
        block = message_ref[pl.ds(96 + r, 32, stride=100), :]
        high = block.astype(jnp.bfloat16).astype(jnp.float32)
        low = block - high
        early.append(jnp.where(lane < 64, high, pltpu.roll(low, 64, 1)))
        late.append(jnp.where(lane < 64, pltpu.roll(high, 64, 1), low))
    operators = jnp.concatenate(early + late, 0).astype(jnp.bfloat16)
    spread_out_ref[...] = jnp.dot(operators, spread_ref[...], preferred_element_type=jnp.float32)

    def load(t, pair):
        value = jnp.concatenate(
            [
                jnp.concatenate(
                    [
                        message_ref[pl.ds((g * 3 + t) * 8 + 2 * pair + side, 32, stride=100), :]
                        for g in range(4)
                    ],
                    0,
                )
                for side in range(2)
            ],
            1,
        )
        high = value.astype(jnp.bfloat16)
        low = (value - high.astype(jnp.float32)).astype(jnp.bfloat16)
        both = jnp.dot(
            forward, jnp.concatenate([high, low], 0), preferred_element_type=jnp.float32
        )
        spectrum_ref[pair % 2] = both[:128] + both[128:]

    def decompose(t, pair):
        for side in range(2):
            r = 2 * pair + side
            at = pl.ds(128 * side, 128)
            for line in range(2):
                field_real = spectrum_ref[pair % 2, pl.ds(32 * line, 32), at]
                field_imag = spectrum_ref[pair % 2, pl.ds(64 + 32 * line, 32), at]
                real_sum = None
                imag_sum = None
                for shift in range(4):
                    weight_real, weight_imag = [
                        spread_out_ref[
                            32 * r : 32 * r + 32, pl.ds(1024 * line + 512 * part + 128 * shift, 128)
                        ]
                        for part in range(2)
                    ]
                    moved_real = pltpu.roll(field_real, 32 * shift, 1) if shift else field_real
                    moved_imag = pltpu.roll(field_imag, 32 * shift, 1) if shift else field_imag
                    term_real = weight_real * moved_real - weight_imag * moved_imag
                    term_imag = weight_real * moved_imag + weight_imag * moved_real
                    real_sum = term_real if real_sum is None else real_sum + term_real
                    imag_sum = term_imag if imag_sum is None else imag_sum + term_imag
                for value, first in ((real_sum, 0), (imag_sum, 64)):
                    high = value.astype(jnp.bfloat16)
                    low = (value - high.astype(jnp.float32)).astype(jnp.bfloat16)
                    decomposed_ref[pair % 2, pl.ds(first + 32 * line, 32), at] = high
                    decomposed_ref[pair % 2, pl.ds(128 + first + 32 * line, 32), at] = low

    def store(t, pair):
        both = jnp.dot(inverse, decomposed_ref[pair % 2], preferred_element_type=jnp.float32)
        wave = both[:128] + both[128:]
        for side in range(2):
            for g in range(4):
                rows = pl.ds(g * 8 + 2 * pair + side, 32, stride=32)
                wave_ref[rows, :] = wave[32 * g : 32 * g + 32, 128 * side : 128 * side + 128]

    def leaving(t):
        return pltpu.make_async_copy(ready_ref.at[t], out_ref.at[:, :, t], sent.at[t])

    for t in range(3):
        load(t, 0)
        for pair in range(4):
            if pair < 3:
                load(t, pair + 1)
            decompose(t, pair)
            store(t, pair)
        ready_ref[t] = wave_ref[...].reshape(32, 4, 8, 128).astype(jnp.bfloat16)
        leaving(t).start()
    for t in range(3):
        leaving(t).wait()


def middle(message, forward, inverse, spread):
    return pl.pallas_call(
        middle_kernel,
        out_shape=jax.ShapeDtypeStruct((32, 4, 3, 8, 128), jnp.bfloat16),
        in_specs=[pl.BlockSpec(memory_space=pltpu.VMEM)] * 4,
        out_specs=pl.BlockSpec(memory_space=pl.ANY),
        scratch_shapes=[
            pltpu.VMEM((1024, 128), jnp.float32),
            pltpu.VMEM((256, 2048), jnp.float32),
            pltpu.VMEM((2, 128, 256), jnp.float32),
            pltpu.VMEM((2, 256, 256), jnp.bfloat16),
            pltpu.VMEM((3, 32, 4, 8, 128), jnp.bfloat16),
            pltpu.SemaphoreType.DMA((3,)),
        ],
    )(
        pltpu.with_memory_space_constraint(message.astype(jnp.float32).reshape(3200, 128), pltpu.VMEM),
        *[pltpu.with_memory_space_constraint(table, pltpu.VMEM) for table in (forward, inverse, spread)],
    )


def outgoing_kernel(live_ref, field_ref, operator_ref, out_ref):
    row = lax.broadcasted_iota(jnp.int32, (128, 128), 0)
    lane = lax.broadcasted_iota(jnp.int32, (128, 128), 1)

    def put_field(part, t):
        for line in range(2):
            for half in range(2):
                live = row + 128 * half < live_ref[line]
                block = jnp.concatenate(
                    [field_ref[0, c, pl.ds(2 * half + line, 32, stride=4), :] for c in range(4)], 0
                )
                block = jnp.where(live, block.T, jnp.float32(0.0))
                for device in range(16):
                    place = 100 * (16 * half + device) + 48 * part + 24 * line + 8 * t
                    out_ref[place : place + 8, :] = block[8 * device : 8 * device + 8]

    def put_operators():
        for half in range(2):
            lines = [operator_ref[pl.ds(2 * half + line, 32, stride=4), :] for line in range(2)]
            block = jnp.concatenate(lines + lines, 0).T
            block = jnp.where(lane < 64, block, pltpu.roll(block, 124, 0))
            for device in range(16):
                place = 100 * (16 * half + device) + 96
                out_ref[place : place + 4, :] = block[8 * device : 8 * device + 4]

    for part in range(2):
        for t in range(3):

            @pl.when(pl.program_id(0) == 3 * part + t)
            def _():
                put_field(part, t)
                if part == 0 and t == 0:
                    put_operators()


def outgoing(field, live_count, decomposer):
    rows = field.reshape(2, 4, 96, 2, 2, 128).transpose(0, 1, 2, 4, 3, 5).reshape(2, 4, 384, 128)
    operator_rows = decomposer.reshape(32, 2, 2, 128).transpose(0, 2, 1, 3).reshape(128, 128)
    tiles = pl.pallas_call(
        outgoing_kernel,
        grid=(6,),
        out_shape=pltpu.VMEM((3200, 128), jnp.float32),
        in_specs=[
            pl.BlockSpec(memory_space=pltpu.SMEM),
            pl.BlockSpec((1, 4, 128, 128), lambda step: (step // 3, 0, step % 3, 0)),
            pl.BlockSpec((128, 128), lambda step: (0, 0)),
        ],
        out_specs=pl.BlockSpec(memory_space=pltpu.VMEM),
    )(live_count, rows, operator_rows)
    return tiles.reshape(32, 25, 4, 128).astype(jnp.float16)


def panel_blocks(reflection):
    panel = reflection[0].reshape(4, 4, 2, 32, 1024).transpose(2, 1, 0, 3, 4).reshape(1024, 1024)
    taken = jnp.arange(1024, dtype=jnp.int32)
    part, line, device, receiver = taken // 512, taken // 256 % 2, taken // 32 % 8, taken % 32
    place = ((device * 2 + part) * 2 + line) * 32 + receiver
    moved = (place[:, None] == taken[None, :]).astype(jnp.bfloat16)
    panel = jnp.dot(panel, moved, preferred_element_type=jnp.float32).astype(jnp.bfloat16)
    return panel.reshape(1024, 8, 128).transpose(1, 0, 2)


def exchanged(blocks):
    rank = lax.axis_index(PLANE)
    received = [lax.dynamic_index_in_dim(blocks, rank, keepdims=False)]
    for distance in range(1, 8):
        block = lax.dynamic_index_in_dim(blocks, rank ^ distance, keepdims=False)
        pairs = [(i, i ^ distance) for i in range(8)]
        received.append(lax.ppermute(block, PLANE, pairs))
    return received


def panel_halves(received):
    rank = lax.axis_index(PLANE)
    core = lax.axis_index("line_2")
    stack = jnp.stack(received)
    halves = []
    for half in (1 - core, core):
        rows = [
            lax.dynamic_slice(stack, (rank ^ source, half * 512, 0), (1, 512, 128))[0]
            for source in range(8)
        ]
        halves.append(jnp.concatenate(rows, 1))
    return halves


def summed(blocks, axis, scale):
    count = lax.axis_size(axis)
    blocks = (blocks * scale).astype(jnp.float16).reshape(count, -1, blocks.shape[-1])
    blocks = lax.all_to_all(blocks, axis, 0, 0, tiled=True)
    return blocks.astype(jnp.float32).sum(axis=0) * (1.0 / scale)


def closing_kernel(blocks_ref, direct_ref, weight_ref, focusing_ref, energies_ref):
    lane = lax.broadcasted_iota(jnp.int32, (32, 128), 1)
    energy = jnp.zeros((32, 128), jnp.float32)
    for part in range(2):
        tiles = []
        for t in range(3):
            at = pl.ds(384 * part + 128 * t, 128)
            tile = blocks_ref[0, :, at] + blocks_ref[1, :, at]
            tile = (tile + blocks_ref[2, :, at] + blocks_ref[3, :, at]) * jnp.float32(8.0)
            energy = energy + tile * tile
            tiles.append(tile)
        for t in range(3):
            natural = None
            for place in range(4):
                chunk = 4 * t + place
                source = tiles[chunk % 3]
                shift = 32 * (place - chunk // 3) % 128
                moved = pltpu.roll(source, shift, 1) if shift else source
                natural = moved if natural is None else jnp.where(lane < 32 * place, natural, moved)
            at = pl.ds(128 * t, 128)
            focusing_ref[:, 0, part, at] = direct_ref[:, 0, part, at] - natural
    total = jnp.sum(energy, axis=1, keepdims=True) * weight_ref[...]
    energies_ref[...] = total.T[:16].reshape(16, 1, 32)


def closing(blocks, direct_wave, weight):
    return pl.pallas_call(
        closing_kernel,
        out_shape=(
            jax.ShapeDtypeStruct((32, 1, 2, 384), jnp.float32),
            pltpu.VMEM((16, 1, 32), jnp.float32),
        ),
        in_specs=[pl.BlockSpec(memory_space=pltpu.VMEM)] * 3,
        out_specs=(pl.BlockSpec(memory_space=pltpu.VMEM), pl.BlockSpec(memory_space=pltpu.VMEM)),
    )(
        pltpu.with_memory_space_constraint(blocks.astype(jnp.float32), pltpu.VMEM),
        pltpu.with_memory_space_constraint(direct_wave, pltpu.VMEM),
        pltpu.with_memory_space_constraint(weight, pltpu.VMEM),
    )


def on_device(field, live_count, line_owner, decomposer, reflection, direct_wave):
    forward, inverse = transform_tables(line_owner)
    total_freqs = lax.axis_size("freq")
    weight = 2.0 * (lax.axis_index("freq") + 1).astype(jnp.float32) / (total_freqs * (total_freqs + 1))
    weight = jnp.full((1, 128), weight)
    message = outgoing(field, live_count, decomposer)
    message, reflection, weight = lax.optimization_barrier((message, reflection, weight))
    message = lax.all_to_all(message, RECEIVER, 0, 0, tiled=True)
    received = exchanged(panel_blocks(reflection))
    wave = middle(message, forward, inverse, spread_table())
    wave = lax.all_to_all(wave, "line_0", 0, 0, tiled=True)
    other_panel, own_panel = panel_halves(received)
    wave = wave.reshape(4, 8, 2, 2, 3, 8, 128).transpose(3, 1, 2, 0, 5, 4, 6).reshape(2, 8, 64, 384)
    stacked = jnp.stack(
        [jnp.concatenate([wave[0], wave[1]], 2), jnp.concatenate([-wave[1], wave[0]], 2)], 1
    ).reshape(1024, 768)
    sent = jnp.dot(other_panel, stacked, preferred_element_type=jnp.float32).astype(jnp.float16)
    sent = lax.ppermute(sent, "line_2", [(0, 1), (1, 0)])
    product = lax.optimization_barrier(
        jnp.dot(own_panel, stacked, preferred_element_type=jnp.float32)
    )
    product = product + sent.astype(jnp.float32)
    product = summed(product, "line_1", 0.5)
    blocks = (product * 0.125).astype(jnp.float16).reshape(4, 32, 768)
    blocks = lax.all_to_all(blocks, "line_0", 0, 0, tiled=True)
    focusing, energies = closing(blocks, direct_wave, weight)
    energies = lax.all_to_all(energies, "freq", 0, 0, tiled=True)
    energy_sum = energies.reshape(16, 32).sum(axis=0)
    trace_energy = jnp.sqrt(energy_sum / 768 + 1e-06)
    return (focusing, trace_energy)


def solution(mesh):
    finer = Mesh(
        mesh.devices.reshape(mesh.shape["freq"], 4, 4, 2), ("freq", "line_0", "line_1", "line_2")
    )
    in_specs = (
        P("freq", None, None, None, LINE, None),
        P(LINE),
        P(),
        P("freq", None, None, None, LINE, None),
        P("freq", None, None, LINE),
        P(LINE, "freq", None, None),
    )
    out_specs = (P(LINE, "freq", None, None), P(LINE))
    return jax.shard_map(
        on_device, mesh=finer, in_specs=in_specs, out_specs=out_specs, check_vma=False
    )
```

```python
import math

import jax
import jax.numpy as jnp
from jax import lax
from jax.experimental import pallas as pl
from jax.experimental.pallas import tpu as pltpu
from jax.sharding import Mesh
from jax.sharding import PartitionSpec as P

LINE = ("line_0", "line_1", "line_2")
RECEIVER = ("line_1", "line_2", "line_0")
PLANE = ("line_1", "line_2")


def by_receiver_owner(values):
    return values.reshape(4, 4, 2, 2).transpose(3, 1, 2, 0).reshape(64)


def by_line_owner(values):
    return values.reshape(32, 2).T.reshape(64)


def phases(wavenum, owner):
    products = wavenum[:, None] * owner[None, :] % 64
    angles = products.astype(jnp.float32) * (2.0 * math.pi / 64)
    return (jnp.cos(angles), jnp.sin(angles))


def in_two_terms(table):
    high = lax.reduce_precision(table, 8, 7)
    low = lax.reduce_precision(table - high, 8, 7)
    high = high.astype(jnp.bfloat16)
    low = low.astype(jnp.bfloat16)
    return jnp.concatenate(
        [jnp.concatenate([high, high], 1), jnp.concatenate([low, low], 1)], 0
    )


def transform_tables(line_owner):
    wavenum = by_receiver_owner(jnp.arange(64, dtype=jnp.int32))
    cosine, sine = phases(wavenum, by_receiver_owner(line_owner))
    forward = jnp.stack([jnp.stack([cosine, sine]), jnp.stack([-sine, cosine])])
    forward = forward.transpose(0, 2, 1, 3).reshape(128, 128)
    cosine, sine = phases(wavenum, by_line_owner(line_owner))
    inverse = jnp.stack([jnp.stack([cosine.T, -sine.T]), jnp.stack([sine.T, cosine.T])]) / 64
    inverse = inverse.reshape(2, 2, 2, 32, 64).transpose(2, 0, 3, 1, 4).reshape(128, 128)
    return in_two_terms(forward), in_two_terms(inverse)


def spread_table():
    row = jnp.arange(128, dtype=jnp.int32)[:, None]
    column = jnp.arange(2048, dtype=jnp.int32)[None, :]
    line, part, target, source = row // 32 % 2, row // 16 % 2, row // 4 % 4, row % 4
    shift, goal = column // 128 % 4, column // 32 % 4
    found = (line == column // 1024) & (part == column // 512 % 2) & (target == goal)
    found = found & (source == (goal - shift) % 4)
    return found.astype(jnp.bfloat16)


def middle_kernel(
    message_ref,
    forward_ref,
    inverse_ref,
    spread_ref,
    out_ref,
    wave_ref,
    spread_out_ref,
    spectrum_ref,
    decomposed_ref,
    ready_ref,
    sent,
):
    forward = forward_ref[...]
    inverse = inverse_ref[...]
    lane = lax.broadcasted_iota(jnp.int32, (32, 128), 1)
    early = []
    late = []
    for r in range(4):
        block = message_ref[pl.ds(96 + r, 32, stride=100), :]
        high = block.astype(jnp.bfloat16).astype(jnp.float32)
        low = block - high
        early.append(jnp.where(lane < 64, high, pltpu.roll(low, 64, 1)))
        late.append(jnp.where(lane < 64, pltpu.roll(high, 64, 1), low))
    operators = jnp.concatenate(early + late, 0).astype(jnp.bfloat16)
    spread_out_ref[...] = jnp.dot(operators, spread_ref[...], preferred_element_type=jnp.float32)

    def load(t, pair):
        value = jnp.concatenate(
            [
                jnp.concatenate(
                    [
                        message_ref[pl.ds((g * 3 + t) * 8 + 2 * pair + side, 32, stride=100), :]
                        for g in range(4)
                    ],
                    0,
                )
                for side in range(2)
            ],
            1,
        )
        high = value.astype(jnp.bfloat16)
        low = (value - high.astype(jnp.float32)).astype(jnp.bfloat16)
        both = jnp.dot(
            forward, jnp.concatenate([high, low], 0), preferred_element_type=jnp.float32
        )
        spectrum_ref[pair % 2] = both[:128] + both[128:]

    def decompose(t, pair):
        for side in range(2):
            r = 2 * pair + side
            at = pl.ds(128 * side, 128)
            for line in range(2):
                field_real = spectrum_ref[pair % 2, pl.ds(32 * line, 32), at]
                field_imag = spectrum_ref[pair % 2, pl.ds(64 + 32 * line, 32), at]
                real_sum = None
                imag_sum = None
                for shift in range(4):
                    weight_real, weight_imag = [
                        spread_out_ref[
                            32 * r : 32 * r + 32, pl.ds(1024 * line + 512 * part + 128 * shift, 128)
                        ]
                        for part in range(2)
                    ]
                    moved_real = pltpu.roll(field_real, 32 * shift, 1) if shift else field_real
                    moved_imag = pltpu.roll(field_imag, 32 * shift, 1) if shift else field_imag
                    term_real = weight_real * moved_real - weight_imag * moved_imag
                    term_imag = weight_real * moved_imag + weight_imag * moved_real
                    real_sum = term_real if real_sum is None else real_sum + term_real
                    imag_sum = term_imag if imag_sum is None else imag_sum + term_imag
                for value, first in ((real_sum, 0), (imag_sum, 64)):
                    high = value.astype(jnp.bfloat16)
                    low = (value - high.astype(jnp.float32)).astype(jnp.bfloat16)
                    decomposed_ref[pair % 2, pl.ds(first + 32 * line, 32), at] = high
                    decomposed_ref[pair % 2, pl.ds(128 + first + 32 * line, 32), at] = low

    def store(t, pair):
        both = jnp.dot(inverse, decomposed_ref[pair % 2], preferred_element_type=jnp.float32)
        wave = both[:128] + both[128:]
        for side in range(2):
            for g in range(4):
                rows = pl.ds(g * 8 + 2 * pair + side, 32, stride=32)
                wave_ref[rows, :] = wave[32 * g : 32 * g + 32, 128 * side : 128 * side + 128]

    def leaving(t):
        return pltpu.make_async_copy(ready_ref.at[t], out_ref.at[:, :, t], sent.at[t])

    for t in range(3):
        load(t, 0)
        for pair in range(4):
            if pair < 3:
                load(t, pair + 1)
            decompose(t, pair)
            store(t, pair)
        ready_ref[t] = wave_ref[...].reshape(32, 4, 8, 128).astype(jnp.bfloat16)
        leaving(t).start()
    for t in range(3):
        leaving(t).wait()


def middle(message, forward, inverse, spread):
    return pl.pallas_call(
        middle_kernel,
        out_shape=jax.ShapeDtypeStruct((32, 4, 3, 8, 128), jnp.bfloat16),
        in_specs=[pl.BlockSpec(memory_space=pltpu.VMEM)] * 4,
        out_specs=pl.BlockSpec(memory_space=pl.ANY),
        scratch_shapes=[
            pltpu.VMEM((1024, 128), jnp.float32),
            pltpu.VMEM((256, 2048), jnp.float32),
            pltpu.VMEM((2, 128, 256), jnp.float32),
            pltpu.VMEM((2, 256, 256), jnp.bfloat16),
            pltpu.VMEM((3, 32, 4, 8, 128), jnp.bfloat16),
            pltpu.SemaphoreType.DMA((3,)),
        ],
    )(
        pltpu.with_memory_space_constraint(message.astype(jnp.float32).reshape(3200, 128), pltpu.VMEM),
        *[pltpu.with_memory_space_constraint(table, pltpu.VMEM) for table in (forward, inverse, spread)],
    )


def outgoing_kernel(live_ref, field_ref, operator_ref, out_ref):
    row = lax.broadcasted_iota(jnp.int32, (128, 128), 0)
    lane = lax.broadcasted_iota(jnp.int32, (128, 128), 1)

    def put_field(part):
        for line in range(2):
            for half in range(2):
                live = row + 128 * half < live_ref[line]
                for t in range(3):
                    block = jnp.concatenate(
                        [
                            field_ref[pl.ds(384 * c + 128 * t + 2 * half + line, 32, stride=4), :]
                            for c in range(4)
                        ],
                        0,
                    )
                    block = jnp.where(live, block.T, jnp.float32(0.0))
                    for device in range(16):
                        place = 100 * (16 * half + device) + 48 * part + 24 * line + 8 * t
                        out_ref[place : place + 8, :] = block[8 * device : 8 * device + 8]

    def put_operators():
        for half in range(2):
            lines = [operator_ref[pl.ds(2 * half + line, 32, stride=4), :] for line in range(2)]
            block = jnp.concatenate(lines + lines, 0).T
            block = jnp.where(lane < 64, block, pltpu.roll(block, 124, 0))
            for device in range(16):
                place = 100 * (16 * half + device) + 96
                out_ref[place : place + 4, :] = block[8 * device : 8 * device + 4]

    @pl.when(pl.program_id(0) == 0)
    def _():
        put_field(0)
        put_operators()

    @pl.when(pl.program_id(0) == 1)
    def _():
        put_field(1)


def outgoing(field, live_count, decomposer):
    rows = field.reshape(2, 4, 96, 2, 2, 128).transpose(0, 1, 2, 4, 3, 5).reshape(3072, 128)
    operator_rows = decomposer.reshape(32, 2, 2, 128).transpose(0, 2, 1, 3).reshape(128, 128)
    tiles = pl.pallas_call(
        outgoing_kernel,
        grid=(2,),
        out_shape=pltpu.VMEM((3200, 128), jnp.float32),
        in_specs=[
            pl.BlockSpec(memory_space=pltpu.SMEM),
            pl.BlockSpec((1536, 128), lambda part: (part, 0)),
            pl.BlockSpec((128, 128), lambda part: (0, 0)),
        ],
        out_specs=pl.BlockSpec(memory_space=pltpu.VMEM),
    )(live_count, rows, operator_rows)
    return tiles.reshape(32, 25, 4, 128).astype(jnp.float16)


def panel_blocks(reflection):
    panel = reflection[0].reshape(4, 4, 2, 32, 1024).transpose(2, 1, 0, 3, 4).reshape(1024, 1024)
    taken = jnp.arange(1024, dtype=jnp.int32)
    part, line, device, receiver = taken // 512, taken // 256 % 2, taken // 32 % 8, taken % 32
    place = ((device * 2 + part) * 2 + line) * 32 + receiver
    moved = (place[:, None] == taken[None, :]).astype(jnp.bfloat16)
    panel = jnp.dot(panel, moved, preferred_element_type=jnp.float32).astype(jnp.bfloat16)
    return panel.reshape(1024, 8, 128).transpose(1, 0, 2)


def exchanged(blocks):
    rank = lax.axis_index(PLANE)
    received = [lax.dynamic_index_in_dim(blocks, rank, keepdims=False)]
    for distance in range(1, 8):
        block = lax.dynamic_index_in_dim(blocks, rank ^ distance, keepdims=False)
        pairs = [(i, i ^ distance) for i in range(8)]
        received.append(lax.ppermute(block, PLANE, pairs))
    return received


def panel_halves(received):
    rank = lax.axis_index(PLANE)
    core = lax.axis_index("line_2")
    stack = jnp.stack(received)
    halves = []
    for half in (1 - core, core):
        rows = [
            lax.dynamic_slice(stack, (rank ^ source, half * 512, 0), (1, 512, 128))[0]
            for source in range(8)
        ]
        halves.append(jnp.concatenate(rows, 1))
    return halves


def summed(blocks, axis, scale):
    count = lax.axis_size(axis)
    blocks = (blocks * scale).astype(jnp.float16).reshape(count, -1, blocks.shape[-1])
    blocks = lax.all_to_all(blocks, axis, 0, 0, tiled=True)
    return blocks.astype(jnp.float32).sum(axis=0) * (1.0 / scale)


def closing_kernel(blocks_ref, direct_ref, weight_ref, focusing_ref, energies_ref):
    lane = lax.broadcasted_iota(jnp.int32, (32, 128), 1)
    energy = jnp.zeros((32, 128), jnp.float32)
    for part in range(2):
        tiles = []
        for t in range(3):
            at = pl.ds(384 * part + 128 * t, 128)
            tile = blocks_ref[0, :, at] + blocks_ref[1, :, at]
            tile = (tile + blocks_ref[2, :, at] + blocks_ref[3, :, at]) * jnp.float32(8.0)
            energy = energy + tile * tile
            tiles.append(tile)
        for t in range(3):
            natural = None
            for place in range(4):
                chunk = 4 * t + place
                source = tiles[chunk % 3]
                shift = 32 * (place - chunk // 3) % 128
                moved = pltpu.roll(source, shift, 1) if shift else source
                natural = moved if natural is None else jnp.where(lane < 32 * place, natural, moved)
            at = pl.ds(128 * t, 128)
            focusing_ref[:, 0, part, at] = direct_ref[:, 0, part, at] - natural
    total = jnp.sum(energy, axis=1, keepdims=True) * weight_ref[...]
    energies_ref[...] = total.T[:16].reshape(16, 1, 32)


def closing(blocks, direct_wave, weight):
    return pl.pallas_call(
        closing_kernel,
        out_shape=(
            jax.ShapeDtypeStruct((32, 1, 2, 384), jnp.float32),
            pltpu.VMEM((16, 1, 32), jnp.float32),
        ),
        in_specs=[pl.BlockSpec(memory_space=pltpu.VMEM)] * 3,
        out_specs=(pl.BlockSpec(memory_space=pltpu.VMEM), pl.BlockSpec(memory_space=pltpu.VMEM)),
    )(
        pltpu.with_memory_space_constraint(blocks.astype(jnp.float32), pltpu.VMEM),
        pltpu.with_memory_space_constraint(direct_wave, pltpu.VMEM),
        pltpu.with_memory_space_constraint(weight, pltpu.VMEM),
    )


def on_device(field, live_count, line_owner, decomposer, reflection, direct_wave):
    forward, inverse = transform_tables(line_owner)
    total_freqs = lax.axis_size("freq")
    weight = 2.0 * (lax.axis_index("freq") + 1).astype(jnp.float32) / (total_freqs * (total_freqs + 1))
    weight = jnp.full((1, 128), weight)
    message = outgoing(field, live_count, decomposer)
    message, reflection, weight = lax.optimization_barrier((message, reflection, weight))
    message = lax.all_to_all(message, RECEIVER, 0, 0, tiled=True)
    received = exchanged(panel_blocks(reflection))
    wave = middle(message, forward, inverse, spread_table())
    wave = lax.all_to_all(wave, "line_0", 0, 0, tiled=True)
    other_panel, own_panel = panel_halves(received)
    wave = wave.reshape(4, 8, 2, 2, 3, 8, 128).transpose(3, 1, 2, 0, 5, 4, 6).reshape(2, 8, 64, 384)
    stacked = jnp.stack(
        [jnp.concatenate([wave[0], wave[1]], 2), jnp.concatenate([-wave[1], wave[0]], 2)], 1
    ).reshape(1024, 768)
    sent = jnp.dot(other_panel, stacked, preferred_element_type=jnp.float32).astype(jnp.float16)
    sent = lax.ppermute(sent, "line_2", [(0, 1), (1, 0)])
    product = lax.optimization_barrier(
        jnp.dot(own_panel, stacked, preferred_element_type=jnp.float32)
    )
    product = product + sent.astype(jnp.float32)
    product = summed(product, "line_1", 0.5)
    blocks = (product * 0.125).astype(jnp.float16).reshape(4, 32, 768)
    blocks = lax.all_to_all(blocks, "line_0", 0, 0, tiled=True)
    focusing, energies = closing(blocks, direct_wave, weight)
    energies = lax.all_to_all(energies, "freq", 0, 0, tiled=True)
    energy_sum = energies.reshape(16, 32).sum(axis=0)
    trace_energy = jnp.sqrt(energy_sum / 768 + 1e-06)
    return (focusing, trace_energy)


def solution(mesh):
    finer = Mesh(
        mesh.devices.reshape(mesh.shape["freq"], 4, 4, 2), ("freq", "line_0", "line_1", "line_2")
    )
    in_specs = (
        P("freq", None, None, None, LINE, None),
        P(LINE),
        P(),
        P("freq", None, None, None, LINE, None),
        P("freq", None, None, LINE),
        P(LINE, "freq", None, None),
    )
    out_specs = (P(LINE, "freq", None, None), P(LINE))
    return jax.shard_map(
        on_device, mesh=finer, in_specs=in_specs, out_specs=out_specs, check_vma=False
    )
```

```python
import math

import jax
import jax.numpy as jnp
from jax import lax
from jax.experimental import pallas as pl
from jax.experimental.pallas import tpu as pltpu
from jax.sharding import Mesh
from jax.sharding import PartitionSpec as P

LINE = ("line_0", "line_1", "line_2")
RECEIVER = ("line_1", "line_2", "line_0")
PLANE = ("line_1", "line_2")


def by_receiver_owner(values):
    return values.reshape(4, 4, 2, 2).transpose(3, 1, 2, 0).reshape(64)


def by_line_owner(values):
    return values.reshape(32, 2).T.reshape(64)


def phases(wavenum, owner):
    products = wavenum[:, None] * owner[None, :] % 64
    angles = products.astype(jnp.float32) * (2.0 * math.pi / 64)
    return (jnp.cos(angles), jnp.sin(angles))


def in_two_terms(table):
    high = lax.reduce_precision(table, 8, 7)
    low = lax.reduce_precision(table - high, 8, 7)
    high = high.astype(jnp.bfloat16)
    low = low.astype(jnp.bfloat16)
    return jnp.concatenate(
        [jnp.concatenate([high, high], 1), jnp.concatenate([low, low], 1)], 0
    )


def transform_tables(line_owner):
    wavenum = by_receiver_owner(jnp.arange(64, dtype=jnp.int32))
    cosine, sine = phases(wavenum, by_receiver_owner(line_owner))
    forward = jnp.stack([jnp.stack([cosine, sine]), jnp.stack([-sine, cosine])])
    forward = forward.transpose(0, 2, 1, 3).reshape(128, 128)
    cosine, sine = phases(wavenum, by_line_owner(line_owner))
    inverse = jnp.stack([jnp.stack([cosine.T, -sine.T]), jnp.stack([sine.T, cosine.T])]) / 64
    inverse = inverse.reshape(2, 2, 2, 32, 64).transpose(2, 0, 3, 1, 4).reshape(128, 128)
    return in_two_terms(forward), in_two_terms(inverse)


def spread_table():
    row = jnp.arange(128, dtype=jnp.int32)[:, None]
    column = jnp.arange(2048, dtype=jnp.int32)[None, :]
    line, part, target, source = row // 32 % 2, row // 16 % 2, row // 4 % 4, row % 4
    shift, goal = column // 128 % 4, column // 32 % 4
    found = (line == column // 1024) & (part == column // 512 % 2) & (target == goal)
    found = found & (source == (goal - shift) % 4)
    return found.astype(jnp.bfloat16)


def middle_kernel(
    message_ref,
    forward_ref,
    inverse_ref,
    spread_ref,
    out_ref,
    wave_ref,
    spread_out_ref,
    spectrum_ref,
    decomposed_ref,
    ready_ref,
    sent,
):
    forward = forward_ref[...]
    inverse = inverse_ref[...]
    lane = lax.broadcasted_iota(jnp.int32, (32, 128), 1)
    early = []
    late = []
    for r in range(4):
        block = message_ref[pl.ds(96 + r, 32, stride=100), :]
        high = block.astype(jnp.bfloat16).astype(jnp.float32)
        low = block - high
        early.append(jnp.where(lane < 64, high, pltpu.roll(low, 64, 1)))
        late.append(jnp.where(lane < 64, pltpu.roll(high, 64, 1), low))
    operators = jnp.concatenate(early + late, 0).astype(jnp.bfloat16)
    spread_out_ref[...] = jnp.dot(operators, spread_ref[...], preferred_element_type=jnp.float32)

    def load(t, pair):
        value = jnp.concatenate(
            [
                jnp.concatenate(
                    [
                        message_ref[pl.ds((g * 3 + t) * 8 + 2 * pair + side, 32, stride=100), :]
                        for g in range(4)
                    ],
                    0,
                )
                for side in range(2)
            ],
            1,
        )
        high = value.astype(jnp.bfloat16)
        low = (value - high.astype(jnp.float32)).astype(jnp.bfloat16)
        both = jnp.dot(
            forward, jnp.concatenate([high, low], 0), preferred_element_type=jnp.float32
        )
        spectrum_ref[pair % 2] = both[:128] + both[128:]

    def decompose(t, pair):
        for side in range(2):
            r = 2 * pair + side
            at = pl.ds(128 * side, 128)
            for line in range(2):
                field_real = spectrum_ref[pair % 2, pl.ds(32 * line, 32), at]
                field_imag = spectrum_ref[pair % 2, pl.ds(64 + 32 * line, 32), at]
                real_sum = None
                imag_sum = None
                for shift in range(4):
                    weight_real, weight_imag = [
                        spread_out_ref[
                            32 * r : 32 * r + 32, pl.ds(1024 * line + 512 * part + 128 * shift, 128)
                        ]
                        for part in range(2)
                    ]
                    moved_real = pltpu.roll(field_real, 32 * shift, 1) if shift else field_real
                    moved_imag = pltpu.roll(field_imag, 32 * shift, 1) if shift else field_imag
                    term_real = weight_real * moved_real - weight_imag * moved_imag
                    term_imag = weight_real * moved_imag + weight_imag * moved_real
                    real_sum = term_real if real_sum is None else real_sum + term_real
                    imag_sum = term_imag if imag_sum is None else imag_sum + term_imag
                for value, first in ((real_sum, 0), (imag_sum, 64)):
                    high = value.astype(jnp.bfloat16)
                    low = (value - high.astype(jnp.float32)).astype(jnp.bfloat16)
                    decomposed_ref[pair % 2, pl.ds(first + 32 * line, 32), at] = high
                    decomposed_ref[pair % 2, pl.ds(128 + first + 32 * line, 32), at] = low

    def store(t, pair):
        both = jnp.dot(inverse, decomposed_ref[pair % 2], preferred_element_type=jnp.float32)
        wave = both[:128] + both[128:]
        for side in range(2):
            for g in range(4):
                rows = pl.ds(g * 8 + 2 * pair + side, 32, stride=32)
                wave_ref[rows, :] = wave[32 * g : 32 * g + 32, 128 * side : 128 * side + 128]

    def leaving(t):
        return pltpu.make_async_copy(ready_ref.at[t], out_ref.at[:, :, t], sent.at[t])

    for t in range(3):
        load(t, 0)
        for pair in range(4):
            if pair < 3:
                load(t, pair + 1)
            decompose(t, pair)
            store(t, pair)
        ready_ref[t] = wave_ref[...].reshape(32, 4, 8, 128).astype(jnp.bfloat16)
        leaving(t).start()
    for t in range(3):
        leaving(t).wait()


def middle(message, forward, inverse, spread):
    return pl.pallas_call(
        middle_kernel,
        out_shape=jax.ShapeDtypeStruct((32, 4, 3, 8, 128), jnp.bfloat16),
        in_specs=[pl.BlockSpec(memory_space=pltpu.VMEM)] * 4,
        out_specs=pl.BlockSpec(memory_space=pl.ANY),
        scratch_shapes=[
            pltpu.VMEM((1024, 128), jnp.float32),
            pltpu.VMEM((256, 2048), jnp.float32),
            pltpu.VMEM((2, 128, 256), jnp.float32),
            pltpu.VMEM((2, 256, 256), jnp.bfloat16),
            pltpu.VMEM((3, 32, 4, 8, 128), jnp.bfloat16),
            pltpu.SemaphoreType.DMA((3,)),
        ],
    )(
        pltpu.with_memory_space_constraint(message.astype(jnp.float32).reshape(3200, 128), pltpu.VMEM),
        *[pltpu.with_memory_space_constraint(table, pltpu.VMEM) for table in (forward, inverse, spread)],
    )


def outgoing_kernel(
    live_ref, field_hbm, operator_hbm, out_ref, field_ref, operator_ref, field_here, operator_here
):
    fetches = [
        pltpu.make_async_copy(field_hbm.at[part], field_ref.at[part], field_here.at[part])
        for part in range(2)
    ]
    operator_fetch = pltpu.make_async_copy(operator_hbm, operator_ref, operator_here)
    operator_fetch.start()
    for fetch in fetches:
        fetch.start()
    row = lax.broadcasted_iota(jnp.int32, (128, 128), 0)
    lane = lax.broadcasted_iota(jnp.int32, (128, 128), 1)

    def put_field(part):
        for line in range(2):
            for half in range(2):
                live = row + 128 * half < live_ref[line]
                for t in range(3):
                    block = jnp.concatenate(
                        [
                            field_ref[part, pl.ds(384 * c + 128 * t + 2 * half + line, 32, stride=4), :]
                            for c in range(4)
                        ],
                        0,
                    )
                    block = jnp.where(live, block.T, jnp.float32(0.0))
                    for device in range(16):
                        place = 100 * (16 * half + device) + 48 * part + 24 * line + 8 * t
                        out_ref[place : place + 8, :] = block[8 * device : 8 * device + 8]

    def put_operators():
        for half in range(2):
            lines = [operator_ref[pl.ds(2 * half + line, 32, stride=4), :] for line in range(2)]
            block = jnp.concatenate(lines + lines, 0).T
            block = jnp.where(lane < 64, block, pltpu.roll(block, 124, 0))
            for device in range(16):
                place = 100 * (16 * half + device) + 96
                out_ref[place : place + 4, :] = block[8 * device : 8 * device + 4]

    operator_fetch.wait()
    put_operators()
    for part in range(2):
        fetches[part].wait()
        put_field(part)


def outgoing(field, live_count, decomposer):
    rows = field.reshape(2, 4, 96, 2, 2, 128).transpose(0, 1, 2, 4, 3, 5).reshape(2, 1536, 128)
    operator_rows = decomposer.reshape(32, 2, 2, 128).transpose(0, 2, 1, 3).reshape(128, 128)
    tiles = pl.pallas_call(
        outgoing_kernel,
        out_shape=pltpu.VMEM((3200, 128), jnp.float32),
        in_specs=[
            pl.BlockSpec(memory_space=pltpu.SMEM),
            pl.BlockSpec(memory_space=pl.ANY),
            pl.BlockSpec(memory_space=pl.ANY),
        ],
        out_specs=pl.BlockSpec(memory_space=pltpu.VMEM),
        scratch_shapes=[
            pltpu.VMEM((2, 1536, 128), jnp.float32),
            pltpu.VMEM((128, 128), jnp.float32),
            pltpu.SemaphoreType.DMA((2,)),
            pltpu.SemaphoreType.DMA,
        ],
    )(live_count, rows, operator_rows)
    return tiles.reshape(32, 25, 4, 128).astype(jnp.float16)


def panel_blocks(reflection):
    panel = reflection[0].reshape(4, 4, 2, 32, 1024).transpose(2, 1, 0, 3, 4).reshape(1024, 1024)
    taken = jnp.arange(1024, dtype=jnp.int32)
    part, line, device, receiver = taken // 512, taken // 256 % 2, taken // 32 % 8, taken % 32
    place = ((device * 2 + part) * 2 + line) * 32 + receiver
    moved = (place[:, None] == taken[None, :]).astype(jnp.bfloat16)
    panel = jnp.dot(panel, moved, preferred_element_type=jnp.float32).astype(jnp.bfloat16)
    return panel.reshape(1024, 8, 128).transpose(1, 0, 2)


def exchanged(blocks):
    rank = lax.axis_index(PLANE)
    received = [lax.dynamic_index_in_dim(blocks, rank, keepdims=False)]
    for distance in range(1, 8):
        block = lax.dynamic_index_in_dim(blocks, rank ^ distance, keepdims=False)
        pairs = [(i, i ^ distance) for i in range(8)]
        received.append(lax.ppermute(block, PLANE, pairs))
    return received


def panel_halves(received):
    rank = lax.axis_index(PLANE)
    core = lax.axis_index("line_2")
    stack = jnp.stack(received)
    halves = []
    for half in (1 - core, core):
        rows = [
            lax.dynamic_slice(stack, (rank ^ source, half * 512, 0), (1, 512, 128))[0]
            for source in range(8)
        ]
        halves.append(jnp.concatenate(rows, 1))
    return halves


def summed(blocks, axis, scale):
    count = lax.axis_size(axis)
    blocks = (blocks * scale).astype(jnp.float16).reshape(count, -1, blocks.shape[-1])
    blocks = lax.all_to_all(blocks, axis, 0, 0, tiled=True)
    return blocks.astype(jnp.float32).sum(axis=0) * (1.0 / scale)


def closing_kernel(blocks_ref, direct_ref, weight_ref, focusing_ref, energies_ref):
    lane = lax.broadcasted_iota(jnp.int32, (32, 128), 1)
    energy = jnp.zeros((32, 128), jnp.float32)
    for part in range(2):
        tiles = []
        for t in range(3):
            at = pl.ds(384 * part + 128 * t, 128)
            tile = blocks_ref[0, :, at] + blocks_ref[1, :, at]
            tile = (tile + blocks_ref[2, :, at] + blocks_ref[3, :, at]) * jnp.float32(8.0)
            energy = energy + tile * tile
            tiles.append(tile)
        for t in range(3):
            natural = None
            for place in range(4):
                chunk = 4 * t + place
                source = tiles[chunk % 3]
                shift = 32 * (place - chunk // 3) % 128
                moved = pltpu.roll(source, shift, 1) if shift else source
                natural = moved if natural is None else jnp.where(lane < 32 * place, natural, moved)
            at = pl.ds(128 * t, 128)
            focusing_ref[:, 0, part, at] = direct_ref[:, 0, part, at] - natural
    total = jnp.sum(energy, axis=1, keepdims=True) * weight_ref[...]
    energies_ref[...] = total.T[:16].reshape(16, 1, 32)


def closing(blocks, direct_wave, weight):
    return pl.pallas_call(
        closing_kernel,
        out_shape=(
            jax.ShapeDtypeStruct((32, 1, 2, 384), jnp.float32),
            pltpu.VMEM((16, 1, 32), jnp.float32),
        ),
        in_specs=[pl.BlockSpec(memory_space=pltpu.VMEM)] * 3,
        out_specs=(pl.BlockSpec(memory_space=pltpu.VMEM), pl.BlockSpec(memory_space=pltpu.VMEM)),
    )(
        pltpu.with_memory_space_constraint(blocks.astype(jnp.float32), pltpu.VMEM),
        pltpu.with_memory_space_constraint(direct_wave, pltpu.VMEM),
        pltpu.with_memory_space_constraint(weight, pltpu.VMEM),
    )


def on_device(field, live_count, line_owner, decomposer, reflection, direct_wave):
    forward, inverse = transform_tables(line_owner)
    total_freqs = lax.axis_size("freq")
    weight = 2.0 * (lax.axis_index("freq") + 1).astype(jnp.float32) / (total_freqs * (total_freqs + 1))
    weight = jnp.full((1, 128), weight)
    message = outgoing(field, live_count, decomposer)
    message, reflection, weight = lax.optimization_barrier((message, reflection, weight))
    message = lax.all_to_all(message, RECEIVER, 0, 0, tiled=True)
    received = exchanged(panel_blocks(reflection))
    wave = middle(message, forward, inverse, spread_table())
    wave = lax.all_to_all(wave, "line_0", 0, 0, tiled=True)
    other_panel, own_panel = panel_halves(received)
    wave = wave.reshape(4, 8, 2, 2, 3, 8, 128).transpose(3, 1, 2, 0, 5, 4, 6).reshape(2, 8, 64, 384)
    stacked = jnp.stack(
        [jnp.concatenate([wave[0], wave[1]], 2), jnp.concatenate([-wave[1], wave[0]], 2)], 1
    ).reshape(1024, 768)
    sent = jnp.dot(other_panel, stacked, preferred_element_type=jnp.float32).astype(jnp.float16)
    sent = lax.ppermute(sent, "line_2", [(0, 1), (1, 0)])
    product = lax.optimization_barrier(
        jnp.dot(own_panel, stacked, preferred_element_type=jnp.float32)
    )
    product = product + sent.astype(jnp.float32)
    product = summed(product, "line_1", 0.5)
    blocks = (product * 0.125).astype(jnp.float16).reshape(4, 32, 768)
    blocks = lax.all_to_all(blocks, "line_0", 0, 0, tiled=True)
    focusing, energies = closing(blocks, direct_wave, weight)
    energies = lax.all_to_all(energies, "freq", 0, 0, tiled=True)
    energy_sum = energies.reshape(16, 32).sum(axis=0)
    trace_energy = jnp.sqrt(energy_sum / 768 + 1e-06)
    return (focusing, trace_energy)


def solution(mesh):
    finer = Mesh(
        mesh.devices.reshape(mesh.shape["freq"], 4, 4, 2), ("freq", "line_0", "line_1", "line_2")
    )
    in_specs = (
        P("freq", None, None, None, LINE, None),
        P(LINE),
        P(),
        P("freq", None, None, None, LINE, None),
        P("freq", None, None, LINE),
        P(LINE, "freq", None, None),
    )
    out_specs = (P(LINE, "freq", None, None), P(LINE))
    return jax.shard_map(
        on_device, mesh=finer, in_specs=in_specs, out_specs=out_specs, check_vma=False
    )
```
